512 devices in a mesh: group: 2 (over core), dp: 64 (over y, x, z_hi), mp: 4 (over z_lo).
Axes of the slice: x: 4, y: 8, z: 8 (z_hi: 2, z_lo: 4; z = z_hi * 4 + z_lo), core: 2. Of those that a mesh axis runs over, the one named last changes fastest.
Arguments:
- x_arrive: bfloat16 [256, 256, 1152], P(('group', 'dp')), may hold values from -6 to 6
- cond_first: int32 [128], P(('group', 'dp')), may hold values 0 or 1
- labels: int32 [128], P(('group', 'dp')), may hold values from 0 to 999
- step_ids: int32 [128], P(('group', 'dp')), may hold values from 0 to 999
- guidance: float32 [1], replicated, may hold values from 2 to 6
- time_table: bfloat16 [1000, 1152], P(None, 'mp'), may hold values from -6 to 6
- class_table: bfloat16 [1001, 1152], P(None, 'mp'), may hold values from -6 to 6
- ada_weight: bfloat16 [1152, 6912], P('mp', 'dp'), may hold values from -0.1875 to 0.1875
- final_ada: bfloat16 [1152, 2304], P('mp'), may hold values from -0.1875 to 0.1875
- qkv_weight: bfloat16 [3, 1152, 1152], P(None, 'dp', 'mp'), may hold values from -2 to 2
- proj_weight: bfloat16 [1152, 1152], P('mp', 'dp'), may hold values from -0.1875 to 0.1875
- fc1_weight: bfloat16 [1152, 4608], P('dp', 'mp'), may hold values from -0.1875 to 0.1875
- fc2_weight: bfloat16 [4608, 1152], P('mp', 'dp'), may hold values from -0.09375 to 0.09375
- out_weight: bfloat16 [1152, 16], replicated, may hold values from -0.1875 to 0.1875
Outputs:
- guided: float32 [128, 4096], P(('group', 'dp'), 'mp')
The draws below stay inside these ranges and needn't reach their ends.
All inputs are finite; a program needn't handle non-finite values. No bound on the sum of `cond_first` on one device may be relied on, other than what follows from the above.
Results may differ from the reference program's by a relative error of at most 0.025.
Values may be sent and summed in bfloat16 or wider, within the bound.
No kernel may reach another device: no remote copies, remote signals or barrier semaphores. Data moves between devices by JAX's collectives and lax.ppermute only.
A program may use at most 64 MiB of HBM per device.

```python
import math
import jax
import jax.numpy as jnp
import numpy as np
from jax import lax

D = 1152
HEADS = 16
FF = 4608
CLASSES = 1000
STEPS = 1000
OUT = 16
TOK = 256
PAIRS = 128
BATCH = 256
N_MP = 4


def draw_qkv_weight(key, part):
    stacked = jax.random.normal(key, (3, D, D), jnp.float32) / math.sqrt(D)
    return jnp.clip(stacked, -2.0, 2.0).astype(jnp.bfloat16)


def plant(values, key, least, top_value):
    index_at = [jax.random.randint(jax.random.fold_in(key, axis), (), 0, length) for axis, length in enumerate(values.shape)]
    widest = values.shape.index(max(values.shape))
    beside = index_at[:widest] + [(index_at[widest] + 1) % values.shape[widest]] + index_at[widest + 1:]
    return values.at[tuple(index_at)].set(least).at[tuple(beside)].set(top_value)


def steps_of(rng, shape, pieces, smallest, high):
    level, own = 1.0, jax.random.fold_in(rng, 6)
    for dim, blocks in pieces:
        heights = jnp.exp(jax.random.uniform(jax.random.fold_in(own, dim), (blocks,), jnp.float32, smallest / len(pieces), high / len(pieces)))
        level = level * jnp.repeat(heights, shape[dim] // blocks).reshape([-1 if axis == dim else 1 for axis in range(len(shape))])
    return level


def rank_table(number_of, skew):
    loads = [(1 << 20) // math.isqrt(standing ** skew) + 1 for standing in range(1, number_of + 1)]
    scale = 1 + sum(loads) // (1 << 30)
    return np.cumsum(np.array([max(1, weight // scale) for weight in loads]))


def skewed_ids(own_key, shape, number_of, slope):
    grid = rank_table(number_of, slope)
    ticket = jax.random.randint(jax.random.fold_in(own_key, 1), shape, 0, int(grid[number_of - 1]))
    grade = jnp.searchsorted(jnp.asarray(grid, jnp.int32), ticket, side="right")
    return jax.random.permutation(jax.random.fold_in(own_key, 2), number_of)[grade].astype(jnp.int32)


def gaussian(key, shape, deviation, reach, cuts=(), held_as=jnp.bfloat16):
    result = jax.random.normal(key, shape, jnp.float32) * deviation
    if len(cuts) > 0:
        result = steps_of(key, shape, cuts, -0.22, 0.18) * result
    return jnp.clip(result, min=-reach, max=reach).astype(held_as)


def setup_inputs(seed: int = 0) -> dict:
    arg_keys = jax.random.split(jax.random.key(seed), 15)
    x_arrive = gaussian(arg_keys[0], (BATCH, TOK, D), 1.0, 6.0, ((0, 128),))
    cond_first = plant((jax.random.randint(arg_keys[1], (PAIRS,), 0, 2) < 1).astype(jnp.int32), jax.random.fold_in(arg_keys[1], 1), 0, 1)
    labels = plant(skewed_ids(arg_keys[2], (PAIRS,), CLASSES, 2), jax.random.fold_in(arg_keys[2], 3), 0, CLASSES - 1).astype(jnp.int32)
    step_ids = plant(jax.random.randint(arg_keys[3], (PAIRS,), 0, STEPS), jax.random.fold_in(arg_keys[3], 1), 0, STEPS - 1).astype(jnp.int32)
    guidance = jnp.clip(jax.random.uniform(arg_keys[4], (1,), jnp.float32, 2.0, 6.0), 2.0, 6.0)
    time_table = gaussian(arg_keys[5], (STEPS, D), 1.0, 6.0, ((1, 4),))
    class_table = gaussian(arg_keys[6], (CLASSES + 1, D), 1.0, 6.0, ((1, 4),))
    ada_weight = gaussian(arg_keys[7], (D, 6 * D), D ** -0.5, 0.1875, ((0, 4), (1, 64)))
    final_ada = gaussian(arg_keys[8], (D, 2 * D), D ** -0.5, 0.1875, ((0, 4),))
    qkv_weight = draw_qkv_weight(jax.random.fold_in(arg_keys[14], 71), 0)
    proj_weight = gaussian(arg_keys[10], (D, D), D ** -0.5, 0.1875, ((0, 4), (1, 64)))
    fc1_weight = gaussian(arg_keys[11], (D, FF), D ** -0.5, 0.1875, ((0, 64), (1, 4)))
    fc2_weight = gaussian(arg_keys[12], (FF, D), FF ** -0.5, 0.09375, ((0, 4), (1, 64)))
    out_weight = gaussian(arg_keys[13], (D, OUT), D ** -0.5, 0.1875)
    return dict(x_arrive=x_arrive, cond_first=cond_first, labels=labels, step_ids=step_ids, guidance=guidance, time_table=time_table, class_table=class_table, ada_weight=ada_weight, final_ada=final_ada, qkv_weight=qkv_weight, proj_weight=proj_weight, fc1_weight=fc1_weight, fc2_weight=fc2_weight, out_weight=out_weight)


def layer_norm(values):
    mean = lax.optimization_barrier(jnp.mean(values, axis=-1, keepdims=True))
    centred = values - mean
    spread = lax.optimization_barrier(jnp.mean(centred * centred, axis=-1, keepdims=True))
    return centred * lax.rsqrt(spread + 1e-06)

def reference(x_arrive, cond_first, labels, step_ids, guidance, time_table, class_table, ada_weight, final_ada, qkv_weight, proj_weight, fc1_weight, fc2_weight, out_weight):
    head_dim = D // HEADS
    rows_all = 2 * TOK
    pair_rows = x_arrive.reshape(PAIRS, 2, TOK, D)

    def one_pair(item):
        rows, flag, label, step = item
        first = flag == 1
        cond_rows = jnp.where(first, rows[0], rows[1])
        uncond_rows = jnp.where(first, rows[1], rows[0])
        images = jnp.stack([cond_rows, uncond_rows]).astype(jnp.float32)
        time_part = time_table[step].astype(jnp.float32)
        class_part = jnp.stack([class_table[label], class_table[CLASSES]]).astype(jnp.float32)
        emb = time_part[None, :] + class_part
        act = jax.nn.silu(emb).astype(jnp.bfloat16)
        mods = jnp.dot(act, ada_weight, preferred_element_type=jnp.float32)
        fmods = jnp.dot(act, final_ada, preferred_element_type=jnp.float32)
        shift_a, scale_a, gate_a, shift_m, scale_m, gate_m = jnp.split(mods, 6, axis=1)
        shift_f, scale_f = jnp.split(fmods, 2, axis=1)
        hidden = (layer_norm(images) * (1.0 + scale_a[:, None]) + shift_a[:, None]).astype(jnp.bfloat16)
        flat = hidden.reshape(rows_all, D)
        query = jnp.dot(flat, qkv_weight[0], preferred_element_type=jnp.float32).astype(jnp.bfloat16)
        keys = jnp.dot(flat, qkv_weight[1], preferred_element_type=jnp.float32).astype(jnp.bfloat16)
        values = jnp.dot(flat, qkv_weight[2], preferred_element_type=jnp.float32).astype(jnp.bfloat16)
        query = query.reshape(2, TOK, HEADS, head_dim).astype(jnp.float32)
        keys = keys.reshape(2, TOK, HEADS, head_dim).astype(jnp.float32)
        values = values.reshape(2, TOK, HEADS, head_dim).astype(jnp.float32)
        scores = jnp.einsum('bqhe,bkhe->bhqk', query, keys) * head_dim ** (-0.5)
        probs = jax.nn.softmax(scores, axis=-1).astype(jnp.bfloat16)
        mixed = jnp.einsum('bhqk,bkhe->bqhe', probs.astype(jnp.float32), values).astype(jnp.bfloat16)
        mixed = mixed.reshape(rows_all, N_MP, D // N_MP).astype(jnp.float32)
        proj_groups = proj_weight.reshape(N_MP, D // N_MP, D).astype(jnp.float32)
        attn_parts = jnp.einsum('rgc,gcd->grd', mixed, proj_groups).astype(jnp.bfloat16)
        attn = lax.optimization_barrier(jnp.sum(attn_parts.astype(jnp.float32), axis=0)).reshape(2, TOK, D)
        first_sum = images + gate_a[:, None] * attn
        hidden_two = (layer_norm(first_sum) * (1.0 + scale_m[:, None]) + shift_m[:, None]).astype(jnp.bfloat16)
        up = jnp.dot(hidden_two.reshape(rows_all, D), fc1_weight, preferred_element_type=jnp.float32)
        gelu_h = jax.nn.gelu(up, approximate=True).astype(jnp.bfloat16)
        gelu_groups = gelu_h.reshape(rows_all, N_MP, FF // N_MP).astype(jnp.float32)
        down_groups = fc2_weight.reshape(N_MP, FF // N_MP, D).astype(jnp.float32)
        mlp_parts = jnp.einsum('rgc,gcd->grd', gelu_groups, down_groups).astype(jnp.bfloat16)
        mlp = lax.optimization_barrier(jnp.sum(mlp_parts.astype(jnp.float32), axis=0)).reshape(2, TOK, D)
        second_sum = first_sum + gate_m[:, None] * mlp
        fin = (layer_norm(second_sum) * (1.0 + scale_f[:, None]) + shift_f[:, None]).astype(jnp.bfloat16)
        noise = jnp.dot(fin.reshape(rows_all, D), out_weight, preferred_element_type=jnp.float32)
        noise = noise.reshape(2, TOK * OUT)
        return noise[1] + guidance[0] * (noise[0] - noise[1])
    return lax.map(one_pair, (pair_rows, cond_first, labels, step_ids))
```

```python
import jax
import jax.numpy as jnp
from jax import lax
from jax.experimental import pallas as pl
from jax.experimental.pallas import tpu as pltpu
from jax.sharding import Mesh
from jax.sharding import PartitionSpec as P

HEADS = 16
CLASSES = 1000
DP = ("dp_0", "dp_1", "dp_2")
GROUP_DP = ("group", "dp_0", "dp_1", "dp_2")
BF16 = jnp.bfloat16
F32 = jnp.float32


def to_everyone(x, axis):
    size = lax.axis_size(axis)
    return lax.all_to_all(jnp.broadcast_to(x[None], (size, *x.shape)), axis, 0, 0, tiled=True)


def shift(x, axis, step):
    size = lax.axis_size(axis)
    return lax.ppermute(x, axis, [(i, (i + step) % size) for i in range(size)])


def swap(x, axis, bit):
    size = lax.axis_size(axis)
    return lax.ppermute(x, axis, [(i, i ^ bit) for i in range(size)])


def gather_y(block):
    pieces = to_everyone(block, "dp_0")
    return pieces.reshape(pieces.shape[0] * pieces.shape[1], pieces.shape[2])


def gather_x(block):
    half = block.shape[0] // 2
    left = shift(block, "dp_1", 1)
    right = shift(block, "dp_1", -1)
    far_top = shift(left[:half], "dp_1", 1)
    far_bottom = shift(right[half:], "dp_1", -1)
    return jnp.concatenate([block, left, right, far_top, far_bottom], axis=0)


def layer_norm(values):
    mean = jnp.mean(values, axis=-1, keepdims=True)
    centred = values - mean
    spread = jnp.mean(centred * centred, axis=-1, keepdims=True)
    return centred * lax.rsqrt(spread + 1e-06)


def dot(a, b):
    return jnp.dot(a, b, preferred_element_type=F32)


def dot_t(a, b):
    return lax.dot_general(a, b, (((1,), (1,)), ((), ())), preferred_element_type=F32)


def attention_body(first_ref, second_ref, out_ref):
    head_dim = first_ref.shape[1] // 6
    scale = head_dim ** (-0.5)
    for side, ref in enumerate((first_ref, second_ref)):
        for head in range(2):
            at = head * head_dim
            query = ref[:, at : at + head_dim]
            keys = ref[:, 2 * head_dim + at : 3 * head_dim + at]
            values = ref[:, 4 * head_dim + at : 5 * head_dim + at]
            scores = dot_t(query, keys) * scale
            top = jnp.max(scores, axis=-1, keepdims=True)
            weights = jnp.exp(scores - top)
            total = jnp.sum(weights, axis=-1, keepdims=True)
            probs = (weights / total).astype(BF16)
            mixed = dot(probs, values).astype(BF16)
            column = (2 * side + head) * head_dim
            out_ref[:, column : column + head_dim] = mixed


def attention(first, second, images, tokens):
    width = first.shape[1]
    return pl.pallas_call(
        attention_body,
        grid=(images,),
        in_specs=[
            pl.BlockSpec((tokens, width), lambda i: (i, 0)),
            pl.BlockSpec((tokens, width), lambda i: (i, 0)),
        ],
        out_specs=pl.BlockSpec((tokens, 2 * width // 3), lambda i: (i, 0)),
        out_shape=jax.ShapeDtypeStruct((images * tokens, 2 * width // 3), BF16),
        name="attention",
    )(first, second)


def on_device(
    x_arrive,
    cond_first,
    labels,
    step_ids,
    guidance,
    time_table,
    class_table,
    ada_weight,
    final_ada,
    qkv_weight,
    proj_weight,
    fc1_weight,
    fc2_weight,
    out_weight,
):
    tokens = x_arrive.shape[1]
    width = x_arrive.shape[2]
    rows = qkv_weight.shape[1]
    quarter = qkv_weight.shape[2]
    core = lax.axis_index("group")
    column = lax.axis_index("dp_1")
    high = lax.axis_index("dp_2")
    place = lax.axis_index("mp")
    n_y, n_x, n_z = (lax.axis_size(axis) for axis in DP)
    n_mp = lax.axis_size("mp")
    half = quarter // 2

    time_part = jnp.take(time_table, step_ids, axis=0).astype(F32)
    class_part = jnp.take(class_table, labels, axis=0).astype(F32)
    null_part = class_table[CLASSES].astype(F32)[None, :]
    acts = jax.nn.silu(jnp.concatenate([time_part + class_part, time_part + null_part])).astype(BF16)
    every_act = to_everyone(acts, DP).reshape(-1, acts.shape[1])

    qkv_first = jnp.where(core == 0, qkv_weight[:, :, :half], qkv_weight[:, :, half:])
    qkv_first = qkv_first.transpose(1, 0, 2).reshape(rows, 3 * half)
    proj_rows = proj_weight.T
    around = to_everyone(jnp.concatenate([qkv_first, proj_rows], axis=1), ("dp_2", "mp"))
    around = around.reshape(n_z, n_mp, rows, 3 * half + quarter)
    own_qkv = lax.dynamic_index_in_dim(around, place, 1, keepdims=False)[:, :, : 3 * half]
    own_proj = lax.dynamic_slice_in_dim(around, core * (n_mp // 2), n_mp // 2, 1)[..., 3 * half :]
    own_proj = own_proj.transpose(0, 2, 1, 3).reshape(n_z, rows, n_mp // 2 * quarter)
    block_a = jnp.concatenate([own_qkv, own_proj], axis=2).reshape(n_z * rows, -1)
    pad = -block_a.shape[1] % 128
    block_a = jnp.pad(block_a, ((0, 0), (0, pad)))

    feed = jnp.stack([fc1_weight, fc2_weight.T])
    near = []
    spots = [(c, z, m) for c in range(2) for z in range(n_z) for m in range(n_mp)]
    number = {spot: i for i, spot in enumerate(spots)}
    for flip in range(n_z):
        pairs = [(number[c, z, m], number[c, z ^ flip, m ^ (2 * c)]) for c, z, m in spots]
        near.append(lax.ppermute(feed, ("group", "dp_2", "mp"), pairs))
    low = jnp.where(high == 0, near[0], near[1])
    up_part = jnp.where(high == 0, near[1], near[0])
    feed = jnp.concatenate([low, up_part], axis=1)

    part_a = gather_x(gather_y(block_a))
    both_a = to_everyone(part_a, "group")
    part_b = gather_x(gather_y(feed[0]))
    other_b = swap(part_b, "group", 1)
    part_c = gather_x(gather_y(feed[1]))
    other_c = swap(part_c, "group", 1)

    mod_part = dot(every_act, ada_weight).astype(BF16)
    mod_part = lax.all_to_all(mod_part, DP, split_axis=0, concat_axis=1, tiled=True)
    final_part = dot(acts, final_ada).astype(BF16)
    mod_parts = to_everyone(jnp.concatenate([mod_part, final_part], axis=1), "mp")

    spot = lax.broadcasted_iota(jnp.int32, (1, width), 1)
    per_x = n_y * n_z * rows
    per_y = n_z * rows
    block = spot // per_x
    offset = jnp.where(block == 1, n_x - 1, jnp.where(block == 2, 1, jnp.where(block == 3, 2, 0)))
    from_x = (column + offset) % n_x
    inside = spot % per_x
    natural = (inside // per_y * n_x + from_x) * per_y + inside % per_y
    order = (lax.broadcasted_iota(jnp.int32, (width, width), 0) == natural).astype(BF16)

    first = cond_first[0] == 1
    cond_rows = jnp.where(first, x_arrive[0], x_arrive[1])
    uncond_rows = jnp.where(first, x_arrive[1], x_arrive[0])
    images = dot(jnp.concatenate([cond_rows, uncond_rows]), order)
    images = images.reshape(2, tokens, width)
    out_local = lax.dot_general(
        order, out_weight, (((0,), (0,)), ((), ())), preferred_element_type=F32
    ).astype(BF16)
    mods = dot(mod_parts.reshape(-1, width), order).reshape(n_mp, 2, -1, 1, width)
    mods = jnp.sum(mods, axis=0)
    shift_a, scale_a, gate_a, shift_m, scale_m, gate_m, shift_f, scale_f = (
        mods[:, i] for i in range(8)
    )

    hidden = (layer_norm(images) * (1.0 + scale_a) + shift_a).astype(BF16)
    hidden = hidden.reshape(2 * tokens, width)
    cut = 3 * half
    qkv_a = dot(hidden, both_a[0, :, :cut]).astype(BF16)
    qkv_b = dot(hidden, both_a[1, :, :cut]).astype(BF16)
    mixed = attention(qkv_a, qkv_b, 2, tokens)
    share = tokens // n_mp
    mixed = mixed.reshape(2, n_mp, share, quarter).transpose(1, 0, 2, 3)
    mixed = lax.all_to_all(mixed.reshape(n_mp, 2 * share, quarter), "mp", 0, 0, tiled=True)
    mixed = mixed.transpose(1, 0, 2).reshape(2 * share, width)
    middle = n_mp // 2 * quarter
    attn = dot_t(mixed[:, :middle], both_a[0, :, cut : cut + middle])
    attn = attn + dot_t(mixed[:, middle:], both_a[1, :, cut : cut + middle])

    own = lax.dynamic_slice_in_dim(images, place * share, share, 1)
    first_sum = own + gate_a * attn.reshape(2, share, width)
    hidden_two = (layer_norm(first_sum) * (1.0 + scale_m) + shift_m).astype(BF16)
    hidden_two = hidden_two.reshape(2 * share, width)
    feed_rows = jnp.concatenate([hidden_two, swap(hidden_two, "mp", 1)])
    gelu_b = jax.nn.gelu(dot(feed_rows, part_b), approximate=True).astype(BF16)
    gelu_c = jax.nn.gelu(dot(feed_rows, other_b), approximate=True).astype(BF16)
    down = dot_t(gelu_b, part_c) + dot_t(gelu_c, other_c)
    from_pair = swap(down[2 * share :].astype(BF16), "mp", 1).astype(F32)
    mlp = (down[: 2 * share] + from_pair).reshape(2, share, width)
    second_sum = first_sum + gate_m * mlp
    fin = (layer_norm(second_sum) * (1.0 + scale_f) + shift_f).astype(BF16)
    noise = dot(fin.reshape(2 * share, width), out_local)
    noise = noise.reshape(2, 1, share * out_weight.shape[1])
    return noise[1] + guidance[0] * (noise[0] - noise[1])


def solution(mesh):
    torus = Mesh(
        mesh.devices.reshape(mesh.shape["group"], 8, 4, 2, mesh.shape["mp"]),
        ("group", "dp_0", "dp_1", "dp_2", "mp"),
    )
    placed = (
        P(GROUP_DP, None, None),
        P(GROUP_DP),
        P(GROUP_DP),
        P(GROUP_DP),
        P(),
        P(None, "mp"),
        P(None, "mp"),
        P("mp", DP),
        P("mp", None),
        P(None, DP, "mp"),
        P("mp", DP),
        P(DP, "mp"),
        P("mp", DP),
        P(),
    )
    return jax.shard_map(
        on_device, mesh=torus, in_specs=placed, out_specs=P(GROUP_DP, "mp"), check_vma=False
    )
```

```python
import jax
import jax.numpy as jnp
from jax import lax
from jax.experimental import pallas as pl
from jax.experimental.pallas import tpu as pltpu
from jax.sharding import Mesh
from jax.sharding import PartitionSpec as P

CLASSES = 1000
DP = ("dp_0", "dp_1", "dp_2")
GROUP_DP = ("group", "dp_0", "dp_1", "dp_2")
BF16 = jnp.bfloat16
F32 = jnp.float32


def to_everyone(x, axis):
    size = lax.axis_size(axis)
    return lax.all_to_all(jnp.broadcast_to(x[None], (size, *x.shape)), axis, 0, 0, tiled=True)


def shift(x, axis, step):
    size = lax.axis_size(axis)
    return lax.ppermute(x, axis, [(i, (i + step) % size) for i in range(size)])


def swap(x, axis, bit):
    size = lax.axis_size(axis)
    return lax.ppermute(x, axis, [(i, i ^ bit) for i in range(size)])


def gather_y(block):
    pieces = to_everyone(block, "dp_0")
    return pieces.reshape(pieces.shape[0] * pieces.shape[1], pieces.shape[2])


def gather_x(block):
    half = block.shape[0] // 2
    left = shift(block, "dp_1", 1)
    right = shift(block, "dp_1", -1)
    far_top = shift(left[:half], "dp_1", 1)
    far_bottom = shift(right[half:], "dp_1", -1)
    return jnp.concatenate([block, left, right, far_top, far_bottom], axis=0)


def by_height(own, other, high):
    own_low = high == 0
    return jnp.concatenate([jnp.where(own_low, own, other), jnp.where(own_low, other, own)])


def lanes_full(x):
    return jnp.pad(x, ((0, 0), (0, -x.shape[1] % 128)))


def layer_norm(values):
    mean = jnp.mean(values, axis=-1, keepdims=True)
    centred = values - mean
    spread = jnp.mean(centred * centred, axis=-1, keepdims=True)
    return centred * lax.rsqrt(spread + 1e-06)


def dot(a, b):
    return jnp.dot(a, b, preferred_element_type=F32)


def dot_t(a, b):
    return lax.dot_general(a, b, (((1,), (1,)), ((), ())), preferred_element_type=F32)


def whole(shape):
    return pl.BlockSpec(shape, lambda *_: (0,) * len(shape))


def attention_body(core_ref, x_ref, shift_ref, scale_ref, mine_ref, other_ref, out_ref):
    images, tokens, _ = x_ref.shape
    pieces, quarter, _ = out_ref.shape
    head_dim = quarter // 4
    share = tokens // pieces
    scale = head_dim ** (-0.5)
    low = core_ref[0] == 0
    for image in range(images):
        x = x_ref[image].astype(F32)
        hidden = (layer_norm(x) * (1.0 + scale_ref[image]) + shift_ref[image]).astype(BF16)
        sides = []
        for ref in (mine_ref, other_ref):
            qkv = dot(hidden, ref[...]).astype(BF16)
            heads = []
            for head in range(2):
                at = head * head_dim
                query = qkv[:, at : at + head_dim]
                keys = qkv[:, 2 * head_dim + at : 3 * head_dim + at]
                values = qkv[:, 4 * head_dim + at : 5 * head_dim + at]
                scores = dot_t(query, keys) * scale
                top = jnp.max(scores, axis=-1, keepdims=True)
                weights = jnp.exp(scores - top)
                total = jnp.sum(weights, axis=-1, keepdims=True)
                probs = (weights / total).astype(BF16)
                mixed = lax.dot_general(
                    values, probs, (((0,), (1,)), ((), ())), preferred_element_type=F32
                )
                heads.append(mixed.astype(BF16))
            sides.append(jnp.concatenate(heads, axis=0))
        first = jnp.where(low, sides[0], sides[1])
        second = jnp.where(low, sides[1], sides[0])
        mixed = jnp.concatenate([first, second], axis=0)
        for piece in range(pieces):
            part = mixed[:, piece * share : (piece + 1) * share]
            out_ref[piece, :, image * share : (image + 1) * share] = part


def attention(core, x, shift_a, scale_a, mine, other, n_mp, quarter):
    images, tokens, width = x.shape
    vector = whole((images, 1, width))
    out_shape = (n_mp, quarter, images * tokens // n_mp)
    return pl.pallas_call(
        attention_body,
        grid_spec=pltpu.PrefetchScalarGridSpec(
            num_scalar_prefetch=1,
            grid=(1,),
            in_specs=[whole(x.shape), vector, vector, whole(mine.shape), whole(other.shape)],
            out_specs=whole(out_shape),
        ),
        out_shape=jax.ShapeDtypeStruct(out_shape, BF16),
        name="attention",
    )(core, x, shift_a, scale_a, mine, other)


def project_body(base_ref, mixed_ref, mine_ref, other_ref, own_ref, gate_ref, shift_ref, scale_ref,
                 sum_ref, hidden_ref, rows_ref):
    quarter = mixed_ref.shape[1]
    base = base_ref[0]
    for i in range(4):
        rows_ref[i * quarter : (i + 1) * quarter] = mixed_ref[base ^ i]
    middle = 2 * quarter
    both = (((0,), (1,)), ((), ()))
    attn = lax.dot_general(
        rows_ref[:middle], mine_ref[:, :middle], both, preferred_element_type=F32
    ) + lax.dot_general(
        rows_ref[middle:], other_ref[:, :middle], both, preferred_element_type=F32
    )
    share = own_ref.shape[1]
    for i in range(2):
        total = own_ref[i].astype(F32) + gate_ref[i] * attn[i * share : (i + 1) * share]
        sum_ref[i] = total
        hidden_ref[i] = (layer_norm(total) * (1.0 + scale_ref[i]) + shift_ref[i]).astype(BF16)


def project(base, mixed, mine, other, own, gate_a, shift_m, scale_m):
    _, share, width = own.shape
    vector = whole((2, 1, width))
    aside = pl.BlockSpec(
        (pl.Element(width), pl.Element(mine.shape[1] - width)), lambda *_: (0, width)
    )
    return pl.pallas_call(
        project_body,
        grid_spec=pltpu.PrefetchScalarGridSpec(
            num_scalar_prefetch=1,
            grid=(1,),
            in_specs=[
                whole(mixed.shape),
                aside,
                aside,
                whole(own.shape),
                vector,
                vector,
                vector,
            ],
            out_specs=[whole(own.shape), whole(own.shape)],
            scratch_shapes=[pltpu.VMEM((4 * mixed.shape[1], 2 * share), BF16)],
        ),
        out_shape=[
            jax.ShapeDtypeStruct(own.shape, F32),
            jax.ShapeDtypeStruct(own.shape, BF16),
        ],
        name="project",
    )(base, mixed, mine, other, own, gate_a, shift_m, scale_m)


def feed_body(own_ref, pair_ref, up_ref, up_other_ref, down_ref, down_other_ref,
              keep_ref, send_ref, rows_ref, sum_ref):
    step = pl.program_id(0)
    half = pl.num_programs(0) // 2
    count = own_ref.shape[0]

    @pl.when(step == 0)
    def _():
        rows_ref[:count] = own_ref[...]
        rows_ref[count:] = pair_ref[...]

    def part(up, down):
        hidden = jax.nn.gelu(dot(rows_ref[...], up[...]), approximate=True).astype(BF16)
        return dot_t(hidden, down[...])

    @pl.when(step == 0)
    def _():
        sum_ref[...] = part(up_ref, down_ref)

    @pl.when((step > 0) & (step < half))
    def _():
        sum_ref[...] += part(up_ref, down_ref)

    @pl.when(step >= half)
    def _():
        sum_ref[...] += part(up_other_ref, down_other_ref)

    @pl.when(step == pl.num_programs(0) - 1)
    def _():
        keep_ref[...] = sum_ref[:count]
        send_ref[...] = sum_ref[count:].astype(BF16)


def feed_forward(own, pair, up, up_other, down, down_other):
    count, width = own.shape
    steps = 3
    piece = width // steps
    first = pl.BlockSpec((width, piece), lambda i: (0, jnp.minimum(i, steps - 1)))
    second = pl.BlockSpec((width, piece), lambda i: (0, jnp.maximum(i - steps, 0)))
    return pl.pallas_call(
        feed_body,
        grid=(2 * steps,),
        in_specs=[whole(own.shape), whole(own.shape), first, second, first, second],
        out_specs=[whole(own.shape), whole(own.shape)],
        out_shape=[
            jax.ShapeDtypeStruct(own.shape, F32),
            jax.ShapeDtypeStruct(own.shape, BF16),
        ],
        scratch_shapes=[pltpu.VMEM((2 * count, width), BF16), pltpu.VMEM((2 * count, width), F32)],
        name="feed_forward",
    )(own, pair, up, up_other, down, down_other)


def finish_body(scale_by_ref, keep_ref, recv_ref, first_ref, gate_ref, shift_ref, scale_ref, out_w_ref, out_ref):
    share = first_ref.shape[1]
    noise = []
    for i in range(2):
        part = slice(i * share, (i + 1) * share)
        mlp = keep_ref[part] + recv_ref[part].astype(F32)
        total = first_ref[i] + gate_ref[i] * mlp
        fin = (layer_norm(total) * (1.0 + scale_ref[i]) + shift_ref[i]).astype(BF16)
        noise.append(dot(fin, out_w_ref[...]))
    out_ref[...] = noise[1] + scale_by_ref[0] * (noise[0] - noise[1])


def finish(guidance, keep, recv, first_sum, gate_m, shift_f, scale_f, out_local):
    _, share, width = first_sum.shape
    vector = whole((2, 1, width))
    return pl.pallas_call(
        finish_body,
        grid_spec=pltpu.PrefetchScalarGridSpec(
            num_scalar_prefetch=1,
            grid=(1,),
            in_specs=[
                whole(keep.shape),
                whole(recv.shape),
                whole(first_sum.shape),
                vector,
                vector,
                vector,
                whole(out_local.shape),
            ],
            out_specs=whole((share, out_local.shape[1])),
        ),
        out_shape=jax.ShapeDtypeStruct((share, out_local.shape[1]), F32),
        name="finish",
    )(guidance, keep, recv, first_sum, gate_m, shift_f, scale_f, out_local)


def on_device(
    x_arrive,
    cond_first,
    labels,
    step_ids,
    guidance,
    time_table,
    class_table,
    ada_weight,
    final_ada,
    qkv_weight,
    proj_weight,
    fc1_weight,
    fc2_weight,
    out_weight,
):
    tokens = x_arrive.shape[1]
    width = x_arrive.shape[2]
    rows = qkv_weight.shape[1]
    quarter = qkv_weight.shape[2]
    core = lax.axis_index("group")
    column = lax.axis_index("dp_1")
    high = lax.axis_index("dp_2")
    place = lax.axis_index("mp")
    n_y, n_x, n_z = (lax.axis_size(axis) for axis in DP)
    n_mp = lax.axis_size("mp")
    half = quarter // 2

    time_part = jnp.take(time_table, step_ids, axis=0).astype(F32)
    class_part = jnp.take(class_table, labels, axis=0).astype(F32)
    null_part = class_table[CLASSES].astype(F32)[None, :]
    acts = jax.nn.silu(jnp.concatenate([time_part + class_part, time_part + null_part])).astype(BF16)
    every_act = to_everyone(acts, DP).reshape(-1, acts.shape[1])

    qkv_own = jnp.where(core == 0, qkv_weight[:, :, :half], qkv_weight[:, :, half:])
    qkv_own = qkv_own.transpose(1, 0, 2).reshape(rows, 3 * half)
    qkv_other = swap(qkv_own, "dp_2", 1)
    qkv_block = lanes_full(by_height(qkv_own, qkv_other, high))

    proj_rows = proj_weight.T
    feed = jnp.concatenate([fc2_weight.T, fc1_weight, proj_rows], axis=1)
    spots = [(c, z, m) for c in range(2) for z in range(n_z) for m in range(n_mp)]
    number = {spot: i for i, spot in enumerate(spots)}

    def fetch(x, flip, along):
        pairs = [(number[c, z, m], number[c, z ^ flip, m ^ (2 * c) ^ along]) for c, z, m in spots]
        return lax.ppermute(x, ("group", "dp_2", "mp"), pairs)

    feed = by_height(fetch(feed, 0, 0), fetch(feed, 1, 0), high)
    proj_beside = by_height(fetch(proj_rows, 0, 1), fetch(proj_rows, 1, 1), high)
    feed = lanes_full(jnp.concatenate([feed, proj_beside], axis=1))
    feed = lax.all_gather(feed, "dp_0", axis=0, tiled=True)

    qkv_block, every_act = lax.optimization_barrier((qkv_block, every_act))
    qkv_block = gather_y(qkv_block)
    qkv_block, every_act = lax.optimization_barrier((qkv_block, every_act))
    part_a = gather_x(qkv_block)
    other_a = swap(part_a, "group", 1)

    mod_part = dot(every_act, ada_weight).astype(BF16)
    mod_part = lax.all_to_all(mod_part, DP, split_axis=0, concat_axis=1, tiled=True)
    feed, mod_part = lax.optimization_barrier((feed, mod_part))
    early = lax.all_gather(feed[:, width:], "dp_1", axis=0, tiled=True)
    other_early = swap(early, "group", 1)
    part_c = lax.all_gather(feed[:, :width], "dp_1", axis=0, tiled=True)
    other_c = swap(part_c, "group", 1)
    final_part = dot(acts, final_ada).astype(BF16)
    mod_parts = to_everyone(jnp.concatenate([mod_part, final_part], axis=1), "mp")

    spot = lax.broadcasted_iota(jnp.int32, (1, width), 1)
    per_x = n_y * n_z * rows
    per_y = n_z * rows
    block = spot // per_x
    inside = spot % per_x
    offset = jnp.where(block == 1, n_x - 1, jnp.where(block == 2, 1, jnp.where(block == 3, 2, 0)))

    def order_of(from_x):
        natural = (inside // per_y * n_x + from_x) * per_y + inside % per_y
        return (lax.broadcasted_iota(jnp.int32, (width, width), 0) == natural).astype(BF16)

    near_order = order_of((column + offset) % n_x)
    order = order_of(block)

    first = cond_first[0] == 1
    cond_rows = jnp.where(first, x_arrive[0], x_arrive[1])
    uncond_rows = jnp.where(first, x_arrive[1], x_arrive[0])
    arrived = jnp.stack([cond_rows, uncond_rows])
    share = tokens // n_mp
    own = lax.dynamic_slice_in_dim(arrived, place * share, share, 1)
    own = dot(own.reshape(-1, width), order).astype(BF16).reshape(2, share, width)
    images = dot(arrived.reshape(-1, width), near_order).astype(BF16)
    images = images.reshape(2, tokens, width)
    out_local = lax.dot_general(
        order, out_weight, (((0,), (0,)), ((), ())), preferred_element_type=F32
    ).astype(BF16)
    mod_parts = mod_parts.reshape(n_mp * 2, -1, width)

    def mods_in(pieces, by):
        count = pieces.shape[1]
        values = dot(pieces.reshape(-1, width), by).reshape(n_mp, 2, count, 1, width)
        values = jnp.sum(values, axis=0)
        return [values[:, i] for i in range(count)]

    shift_a, scale_a = mods_in(mod_parts[:, :2], near_order)
    gate_a, shift_m, scale_m, gate_m, shift_f, scale_f = mods_in(mod_parts[:, 2:], order)

    cores = core.reshape(1).astype(jnp.int32)
    mixed = attention(cores, images, shift_a, scale_a, part_a, other_a, n_mp, quarter)
    mixed = lax.all_to_all(mixed, "mp", 0, 0, tiled=True)
    base = (place ^ (2 * core)).reshape(1).astype(jnp.int32)
    first_sum, hidden_two = project(base, mixed, early, other_early, own, gate_a, shift_m, scale_m)
    hidden_two = hidden_two.reshape(2 * share, width)
    pair = swap(hidden_two, "mp", 1)
    keep, send = feed_forward(hidden_two, pair, early, other_early, part_c, other_c)
    recv = swap(send, "mp", 1)
    guided = finish(guidance, keep, recv, first_sum, gate_m, shift_f, scale_f, out_local)
    return guided.reshape(1, share * out_weight.shape[1])


def solution(mesh):
    torus = Mesh(
        mesh.devices.reshape(mesh.shape["group"], 8, 4, 2, mesh.shape["mp"]),
        ("group", "dp_0", "dp_1", "dp_2", "mp"),
    )
    placed = (
        P(GROUP_DP, None, None),
        P(GROUP_DP),
        P(GROUP_DP),
        P(GROUP_DP),
        P(),
        P(None, "mp"),
        P(None, "mp"),
        P("mp", DP),
        P("mp", None),
        P(None, DP, "mp"),
        P("mp", DP),
        P(DP, "mp"),
        P("mp", DP),
        P(),
    )
    return jax.shard_map(
        on_device, mesh=torus, in_specs=placed, out_specs=P(GROUP_DP, "mp"), check_vma=False
    )
```

```python
import jax
import jax.numpy as jnp
from jax import lax
from jax.experimental import pallas as pl
from jax.experimental.pallas import tpu as pltpu
from jax.sharding import Mesh
from jax.sharding import PartitionSpec as P

CLASSES = 1000
DP = ("dp_0", "dp_1", "dp_2")
GROUP_DP = ("group", "dp_0", "dp_1", "dp_2")
BF16 = jnp.bfloat16
F32 = jnp.float32


def to_everyone(x, axis):
    size = lax.axis_size(axis)
    return lax.all_to_all(jnp.broadcast_to(x[None], (size, *x.shape)), axis, 0, 0, tiled=True)


def shift(x, axis, step):
    size = lax.axis_size(axis)
    return lax.ppermute(x, axis, [(i, (i + step) % size) for i in range(size)])


def swap(x, axis, bit):
    size = lax.axis_size(axis)
    return lax.ppermute(x, axis, [(i, i ^ bit) for i in range(size)])


def gather_y(block):
    pieces = to_everyone(block, "dp_0")
    return pieces.reshape(pieces.shape[0] * pieces.shape[1], pieces.shape[2])


def gather_x(block):
    half = block.shape[0] // 2
    left = shift(block, "dp_1", 1)
    right = shift(block, "dp_1", -1)
    far_top = shift(left[:half], "dp_1", 1)
    far_bottom = shift(right[half:], "dp_1", -1)
    return jnp.concatenate([block, left, right, far_top, far_bottom], axis=0)


def by_height(own, other, high):
    own_low = high == 0
    return jnp.concatenate([jnp.where(own_low, own, other), jnp.where(own_low, other, own)])


def lanes_full(x):
    return jnp.pad(x, ((0, 0), (0, -x.shape[1] % 128)))


def layer_norm(values):
    mean = jnp.mean(values, axis=-1, keepdims=True)
    centred = values - mean
    spread = jnp.mean(centred * centred, axis=-1, keepdims=True)
    return centred * lax.rsqrt(spread + 1e-06)


def dot(a, b):
    return jnp.dot(a, b, preferred_element_type=F32)


def dot_t(a, b):
    return lax.dot_general(a, b, (((1,), (1,)), ((), ())), preferred_element_type=F32)


def whole(shape):
    return pl.BlockSpec(shape, lambda *_: (0,) * len(shape))


def attention_body(core_ref, x_ref, shift_ref, scale_ref, mine_ref, other_ref, out_ref):
    images, tokens, _ = x_ref.shape
    pieces, quarter, _ = out_ref.shape
    head_dim = quarter // 4
    share = tokens // pieces
    scale = head_dim ** (-0.5)
    low = core_ref[0] == 0
    for image in range(images):
        x = x_ref[image].astype(F32)
        hidden = (layer_norm(x) * (1.0 + scale_ref[image]) + shift_ref[image]).astype(BF16)
        sides = []
        for ref in (mine_ref, other_ref):
            qkv = dot(hidden, ref[:, : 6 * head_dim]).astype(BF16)
            heads = []
            for head in range(2):
                at = head * head_dim
                query = qkv[:, at : at + head_dim]
                keys = qkv[:, 2 * head_dim + at : 3 * head_dim + at]
                values = qkv[:, 4 * head_dim + at : 5 * head_dim + at]
                scores = dot_t(query, keys) * scale
                top = jnp.max(scores, axis=-1, keepdims=True)
                weights = jnp.exp(scores - top)
                total = jnp.sum(weights, axis=-1, keepdims=True)
                probs = (weights / total).astype(BF16)
                mixed = lax.dot_general(
                    values, probs, (((0,), (1,)), ((), ())), preferred_element_type=F32
                )
                heads.append(mixed.astype(BF16))
            sides.append(jnp.concatenate(heads, axis=0))
        first = jnp.where(low, sides[0], sides[1])
        second = jnp.where(low, sides[1], sides[0])
        mixed = jnp.concatenate([first, second], axis=0)
        for piece in range(pieces):
            part = mixed[:, piece * share : (piece + 1) * share]
            out_ref[piece, :, image * share : (image + 1) * share] = part


def attention(core, x, shift_a, scale_a, mine, other, n_mp, quarter):
    images, tokens, width = x.shape
    vector = whole((images, 1, width))
    out_shape = (n_mp, quarter, images * tokens // n_mp)
    return pl.pallas_call(
        attention_body,
        grid_spec=pltpu.PrefetchScalarGridSpec(
            num_scalar_prefetch=1,
            grid=(1,),
            in_specs=[whole(x.shape), vector, vector, whole(mine.shape), whole(other.shape)],
            out_specs=whole(out_shape),
        ),
        out_shape=jax.ShapeDtypeStruct(out_shape, BF16),
        name="attention",
    )(core, x, shift_a, scale_a, mine, other)


def project_body(base_ref, mixed_ref, mine_ref, other_ref, change_ref, own_ref, gate_ref, shift_ref, scale_ref,
                 sum_ref, hidden_ref, rows_ref):
    quarter = mixed_ref.shape[1]
    start = 3 * quarter // 2
    lead = start % 128
    base = base_ref[0]
    rows_ref[...] = jnp.zeros(rows_ref.shape, BF16)
    for i in range(4):
        at = lead + i % 2 * quarter
        rows_ref[i // 2, at : at + quarter] = mixed_ref[base ^ i]
    both = (((0,), (1,)), ((), ()))
    attn = lax.dot_general(
        rows_ref[0], mine_ref[:, start - lead :], both, preferred_element_type=F32
    ) + lax.dot_general(
        rows_ref[1], other_ref[:, start - lead :], both, preferred_element_type=F32
    )
    share = own_ref.shape[1]
    for i in range(2):
        total = own_ref[i].astype(F32) + gate_ref[i] * attn[i * share : (i + 1) * share]
        sum_ref[i] = total
        hidden = (layer_norm(total) * (1.0 + scale_ref[i]) + shift_ref[i]).astype(BF16)
        hidden_ref[i] = dot_t(hidden, change_ref[...]).astype(BF16)


def project(base, mixed, mine, other, change, own, gate_a, shift_m, scale_m):
    _, share, width = own.shape
    vector = whole((2, 1, width))
    start = 3 * mixed.shape[1] // 2
    depth = mine.shape[1] - start // 128 * 128
    return pl.pallas_call(
        project_body,
        grid_spec=pltpu.PrefetchScalarGridSpec(
            num_scalar_prefetch=1,
            grid=(1,),
            in_specs=[
                whole(mixed.shape),
                whole(mine.shape),
                whole(other.shape),
                whole(change.shape),
                whole(own.shape),
                vector,
                vector,
                vector,
            ],
            out_specs=[whole(own.shape), whole(own.shape)],
            scratch_shapes=[pltpu.VMEM((2, depth, 2 * share), BF16)],
        ),
        out_shape=[
            jax.ShapeDtypeStruct(own.shape, F32),
            jax.ShapeDtypeStruct(own.shape, BF16),
        ],
        name="project",
    )(base, mixed, mine, other, change, own, gate_a, shift_m, scale_m)


def feed_body(own_ref, pair_ref, up_ref, up_other_ref, down_ref, down_other_ref,
              keep_ref, send_ref, rows_ref, sum_ref):
    step = pl.program_id(0)
    half = pl.num_programs(0) // 2
    count = own_ref.shape[0]

    @pl.when(step == 0)
    def _():
        rows_ref[:count] = own_ref[...]
        rows_ref[count:] = pair_ref[...]

    def part(up, down):
        hidden = jax.nn.gelu(dot(rows_ref[...], up[...]), approximate=True).astype(BF16)
        return dot_t(hidden, down[...])

    @pl.when(step == 0)
    def _():
        sum_ref[...] = part(up_ref, down_ref)

    @pl.when((step > 0) & (step < half))
    def _():
        sum_ref[...] += part(up_ref, down_ref)

    @pl.when(step >= half)
    def _():
        sum_ref[...] += part(up_other_ref, down_other_ref)

    @pl.when(step == pl.num_programs(0) - 1)
    def _():
        keep_ref[...] = sum_ref[:count]
        send_ref[...] = sum_ref[count:].astype(BF16)


def feed_forward(own, pair, up, up_other, down, down_other):
    count, width = own.shape
    steps = 3
    piece = width // steps
    first = pl.BlockSpec((width, piece), lambda i: (0, jnp.minimum(i, steps - 1)))
    second = pl.BlockSpec((width, piece), lambda i: (0, jnp.maximum(i - steps, 0)))
    return pl.pallas_call(
        feed_body,
        grid=(2 * steps,),
        in_specs=[whole(own.shape), whole(own.shape), first, second, first, second],
        out_specs=[whole(own.shape), whole(own.shape)],
        out_shape=[
            jax.ShapeDtypeStruct(own.shape, F32),
            jax.ShapeDtypeStruct(own.shape, BF16),
        ],
        scratch_shapes=[pltpu.VMEM((2 * count, width), BF16), pltpu.VMEM((2 * count, width), F32)],
        name="feed_forward",
    )(own, pair, up, up_other, down, down_other)


def finish_body(scale_by_ref, keep_ref, recv_ref, first_ref, gate_ref, shift_ref, scale_ref, out_w_ref, out_ref):
    share = first_ref.shape[1]
    noise = []
    for i in range(2):
        part = slice(i * share, (i + 1) * share)
        mlp = keep_ref[part] + recv_ref[part].astype(F32)
        total = first_ref[i] + gate_ref[i] * mlp
        fin = (layer_norm(total) * (1.0 + scale_ref[i]) + shift_ref[i]).astype(BF16)
        noise.append(dot(fin, out_w_ref[...]))
    out_ref[...] = noise[1] + scale_by_ref[0] * (noise[0] - noise[1])


def finish(guidance, keep, recv, first_sum, gate_m, shift_f, scale_f, out_local):
    _, share, width = first_sum.shape
    vector = whole((2, 1, width))
    return pl.pallas_call(
        finish_body,
        grid_spec=pltpu.PrefetchScalarGridSpec(
            num_scalar_prefetch=1,
            grid=(1,),
            in_specs=[
                whole(keep.shape),
                whole(recv.shape),
                whole(first_sum.shape),
                vector,
                vector,
                vector,
                whole(out_local.shape),
            ],
            out_specs=whole((share, out_local.shape[1])),
        ),
        out_shape=jax.ShapeDtypeStruct((share, out_local.shape[1]), F32),
        name="finish",
    )(guidance, keep, recv, first_sum, gate_m, shift_f, scale_f, out_local)


def on_device(
    x_arrive,
    cond_first,
    labels,
    step_ids,
    guidance,
    time_table,
    class_table,
    ada_weight,
    final_ada,
    qkv_weight,
    proj_weight,
    fc1_weight,
    fc2_weight,
    out_weight,
):
    tokens = x_arrive.shape[1]
    width = x_arrive.shape[2]
    rows = qkv_weight.shape[1]
    quarter = qkv_weight.shape[2]
    core = lax.axis_index("group")
    column = lax.axis_index("dp_1")
    high = lax.axis_index("dp_2")
    place = lax.axis_index("mp")
    n_y, n_x, n_z = (lax.axis_size(axis) for axis in DP)
    n_mp = lax.axis_size("mp")
    half = quarter // 2

    time_part = jnp.take(time_table, step_ids, axis=0).astype(F32)
    class_part = jnp.take(class_table, labels, axis=0).astype(F32)
    null_part = class_table[CLASSES].astype(F32)[None, :]
    acts = jax.nn.silu(jnp.concatenate([time_part + class_part, time_part + null_part])).astype(BF16)
    every_act = to_everyone(acts, DP).reshape(-1, acts.shape[1])

    qkv_own = jnp.where(core == 0, qkv_weight[:, :, :half], qkv_weight[:, :, half:])
    qkv_own = qkv_own.transpose(1, 0, 2).reshape(rows, 3 * half)
    qkv_other = swap(qkv_own, "dp_2", 1)
    qkv_block = by_height(qkv_own, qkv_other, high)

    proj_rows = proj_weight.T
    feed = jnp.concatenate([fc2_weight.T, fc1_weight, proj_rows], axis=1)
    spots = [(c, z, m) for c in range(2) for z in range(n_z) for m in range(n_mp)]
    number = {spot: i for i, spot in enumerate(spots)}

    def fetch(x, flip, along):
        pairs = [(number[c, z, m], number[c, z ^ flip, m ^ (2 * c) ^ along]) for c, z, m in spots]
        return lax.ppermute(x, ("group", "dp_2", "mp"), pairs)

    feed = by_height(fetch(feed, 0, 0), fetch(feed, 1, 0), high)
    proj_beside = by_height(fetch(proj_rows, 0, 1), fetch(proj_rows, 1, 1), high)
    part_a = lanes_full(jnp.concatenate([qkv_block, feed[:, 2 * width :], proj_beside], axis=1))
    part_a, every_act = lax.optimization_barrier((part_a, every_act))
    part_a = gather_y(part_a)
    part_a, every_act = lax.optimization_barrier((part_a, every_act))
    part_a = gather_x(part_a)
    other_a = swap(part_a, "group", 1)

    feed = lax.all_gather(feed[:, : 2 * width], "dp_0", axis=0, tiled=True)
    part_b = lax.all_gather(feed[:, width:], "dp_1", axis=0, tiled=True)
    other_b = swap(part_b, "group", 1)
    part_c = gather_x(feed[:, :width])
    other_c = swap(part_c, "group", 1)

    mod_part = dot(every_act, ada_weight).astype(BF16)
    mod_part = lax.all_to_all(mod_part, DP, split_axis=0, concat_axis=1, tiled=True)
    final_part = dot(acts, final_ada).astype(BF16)
    mod_parts = to_everyone(jnp.concatenate([mod_part, final_part], axis=1), "mp")

    spot = lax.broadcasted_iota(jnp.int32, (1, width), 1)
    per_x = n_y * n_z * rows
    per_y = n_z * rows
    block = spot // per_x
    inside = spot % per_x
    offset = jnp.where(block == 1, n_x - 1, jnp.where(block == 2, 1, jnp.where(block == 3, 2, 0)))

    from_x = (column + offset) % n_x
    final = (inside // per_y * n_x + from_x) * per_y + inside % per_y
    order = (lax.broadcasted_iota(jnp.int32, (width, width), 0) == final).astype(BF16)
    up_natural = (inside // per_y * n_x + block) * per_y + inside % per_y
    change = (up_natural.reshape(width, 1) == final).astype(BF16)

    first = cond_first[0] == 1
    cond_rows = jnp.where(first, x_arrive[0], x_arrive[1])
    uncond_rows = jnp.where(first, x_arrive[1], x_arrive[0])
    arrived = jnp.stack([cond_rows, uncond_rows])
    share = tokens // n_mp
    own = lax.dynamic_slice_in_dim(arrived, place * share, share, 1)
    own = dot(own.reshape(-1, width), order).astype(BF16).reshape(2, share, width)
    images = dot(arrived.reshape(-1, width), order).astype(BF16)
    images = images.reshape(2, tokens, width)
    out_local = lax.dot_general(
        order, out_weight, (((0,), (0,)), ((), ())), preferred_element_type=F32
    ).astype(BF16)
    mod_parts = mod_parts.reshape(n_mp * 2, -1, width)

    def mods_in(pieces, by):
        count = pieces.shape[1]
        values = dot(pieces.reshape(-1, width), by).reshape(n_mp, 2, count, 1, width)
        values = jnp.sum(values, axis=0)
        return [values[:, i] for i in range(count)]

    shift_a, scale_a = mods_in(mod_parts[:, :2], order)
    gate_a, shift_m, scale_m, gate_m, shift_f, scale_f = mods_in(mod_parts[:, 2:], order)

    cores = core.reshape(1).astype(jnp.int32)
    mixed = attention(cores, images, shift_a, scale_a, part_a, other_a, n_mp, quarter)
    mixed = lax.all_to_all(mixed, "mp", 0, 0, tiled=True)
    base = (place ^ (2 * core)).reshape(1).astype(jnp.int32)
    first_sum, hidden_two = project(base, mixed, part_a, other_a, change, own, gate_a, shift_m, scale_m)
    hidden_two = hidden_two.reshape(2 * share, width)
    pair = swap(hidden_two, "mp", 1)
    keep, send = feed_forward(hidden_two, pair, part_b, other_b, part_c, other_c)
    recv = swap(send, "mp", 1)
    guided = finish(guidance, keep, recv, first_sum, gate_m, shift_f, scale_f, out_local)
    return guided.reshape(1, share * out_weight.shape[1])


def solution(mesh):
    torus = Mesh(
        mesh.devices.reshape(mesh.shape["group"], 8, 4, 2, mesh.shape["mp"]),
        ("group", "dp_0", "dp_1", "dp_2", "mp"),
    )
    placed = (
        P(GROUP_DP, None, None),
        P(GROUP_DP),
        P(GROUP_DP),
        P(GROUP_DP),
        P(),
        P(None, "mp"),
        P(None, "mp"),
        P("mp", DP),
        P("mp", None),
        P(None, DP, "mp"),
        P("mp", DP),
        P(DP, "mp"),
        P("mp", DP),
        P(),
    )
    return jax.shard_map(
        on_device, mesh=torus, in_specs=placed, out_specs=P(GROUP_DP, "mp"), check_vma=False
    )
```

```python
import jax
import jax.numpy as jnp
from jax import lax
from jax.experimental import pallas as pl
from jax.experimental.pallas import tpu as pltpu
from jax.sharding import Mesh
from jax.sharding import PartitionSpec as P

CLASSES = 1000
DP = ("dp_0", "dp_1", "dp_2")
GROUP_DP = ("group", "dp_0", "dp_1", "dp_2")
BF16 = jnp.bfloat16
F32 = jnp.float32


def to_everyone(x, axis):
    size = lax.axis_size(axis)
    return lax.all_to_all(jnp.broadcast_to(x[None], (size, *x.shape)), axis, 0, 0, tiled=True)


def shift(x, axis, step):
    size = lax.axis_size(axis)
    return lax.ppermute(x, axis, [(i, (i + step) % size) for i in range(size)])


def swap(x, axis, bit):
    size = lax.axis_size(axis)
    return lax.ppermute(x, axis, [(i, i ^ bit) for i in range(size)])


def gather_y(block):
    pieces = to_everyone(block, "dp_0")
    return pieces.reshape(pieces.shape[0] * pieces.shape[1], pieces.shape[2])


def gather_x(block):
    half = block.shape[0] // 2
    left = shift(block, "dp_1", 1)
    right = shift(block, "dp_1", -1)
    far_top = shift(left[:half], "dp_1", 1)
    far_bottom = shift(right[half:], "dp_1", -1)
    return jnp.concatenate([block, left, right, far_top, far_bottom], axis=0)


def by_height(own, other, high):
    own_low = high == 0
    return jnp.concatenate([jnp.where(own_low, own, other), jnp.where(own_low, other, own)])


def lanes_full(x):
    return jnp.pad(x, ((0, 0), (0, -x.shape[1] % 128)))


def layer_norm(values):
    mean = jnp.mean(values, axis=-1, keepdims=True)
    centred = values - mean
    spread = jnp.mean(centred * centred, axis=-1, keepdims=True)
    return centred * lax.rsqrt(spread + 1e-06)


def dot(a, b):
    return jnp.dot(a, b, preferred_element_type=F32)


def dot_t(a, b):
    return lax.dot_general(a, b, (((1,), (1,)), ((), ())), preferred_element_type=F32)


def whole(shape):
    return pl.BlockSpec(shape, lambda *_: (0,) * len(shape))


def attention_body(core_ref, x_ref, shift_ref, scale_ref, mine_ref, other_ref, out_ref):
    images, tokens, _ = x_ref.shape
    pieces, quarter, _ = out_ref.shape
    head_dim = quarter // 4
    share = tokens // pieces
    scale = head_dim ** (-0.5)
    low = core_ref[0] == 0
    for image in range(images):
        x = x_ref[image].astype(F32)
        hidden = (layer_norm(x) * (1.0 + scale_ref[image]) + shift_ref[image]).astype(BF16)
        sides = []
        for ref in (mine_ref, other_ref):
            qkv = dot(hidden, ref[:, : 6 * head_dim]).astype(BF16)
            heads = []
            for head in range(2):
                at = head * head_dim
                query = qkv[:, at : at + head_dim]
                keys = qkv[:, 2 * head_dim + at : 3 * head_dim + at]
                values = qkv[:, 4 * head_dim + at : 5 * head_dim + at]
                scores = dot_t(query, keys) * scale
                top = jnp.max(scores, axis=-1, keepdims=True)
                weights = jnp.exp(scores - top)
                total = jnp.sum(weights, axis=-1, keepdims=True)
                probs = (weights * (1.0 / total)).astype(BF16)
                mixed = lax.dot_general(
                    values, probs, (((0,), (1,)), ((), ())), preferred_element_type=F32
                )
                heads.append(mixed.astype(BF16))
            sides.append(jnp.concatenate(heads, axis=0))
        first = jnp.where(low, sides[0], sides[1])
        second = jnp.where(low, sides[1], sides[0])
        mixed = jnp.concatenate([first, second], axis=0)
        for piece in range(pieces):
            part = mixed[:, piece * share : (piece + 1) * share]
            out_ref[piece, :, image * share : (image + 1) * share] = part


def attention(core, x, shift_a, scale_a, mine, other, n_mp, quarter):
    images, tokens, width = x.shape
    vector = whole((images, 1, width))
    out_shape = (n_mp, quarter, images * tokens // n_mp)
    return pl.pallas_call(
        attention_body,
        grid_spec=pltpu.PrefetchScalarGridSpec(
            num_scalar_prefetch=1,
            grid=(1,),
            in_specs=[whole(x.shape), vector, vector, whole(mine.shape), whole(other.shape)],
            out_specs=whole(out_shape),
        ),
        out_shape=jax.ShapeDtypeStruct(out_shape, BF16),
        name="attention",
    )(core, x, shift_a, scale_a, mine, other)


def project_body(base_ref, mixed_ref, mine_ref, other_ref, change_ref, own_ref, gate_ref, shift_ref, scale_ref,
                 sum_ref, hidden_ref, rows_ref):
    quarter = mixed_ref.shape[1]
    start = 3 * quarter // 2
    lead = start % 128
    base = base_ref[0]
    rows_ref[...] = jnp.zeros(rows_ref.shape, BF16)
    for i in range(4):
        at = lead + i % 2 * quarter
        rows_ref[i // 2, at : at + quarter] = mixed_ref[base ^ i]
    both = (((0,), (1,)), ((), ()))
    attn = lax.dot_general(
        rows_ref[0], mine_ref[:, start - lead :], both, preferred_element_type=F32
    ) + lax.dot_general(
        rows_ref[1], other_ref[:, start - lead :], both, preferred_element_type=F32
    )
    attn = dot(attn.astype(BF16), change_ref[...])
    share = own_ref.shape[1]
    for i in range(2):
        total = own_ref[i].astype(F32) + gate_ref[i] * attn[i * share : (i + 1) * share]
        sum_ref[i] = total
        hidden_ref[i] = (layer_norm(total) * (1.0 + scale_ref[i]) + shift_ref[i]).astype(BF16)


def project(base, mixed, mine, other, change, own, gate_a, shift_m, scale_m):
    _, share, width = own.shape
    vector = whole((2, 1, width))
    start = 3 * mixed.shape[1] // 2
    depth = mine.shape[1] - start // 128 * 128
    return pl.pallas_call(
        project_body,
        grid_spec=pltpu.PrefetchScalarGridSpec(
            num_scalar_prefetch=1,
            grid=(1,),
            in_specs=[
                whole(mixed.shape),
                whole(mine.shape),
                whole(other.shape),
                whole(change.shape),
                whole(own.shape),
                vector,
                vector,
                vector,
            ],
            out_specs=[whole(own.shape), whole(own.shape)],
            scratch_shapes=[pltpu.VMEM((2, depth, 2 * share), BF16)],
        ),
        out_shape=[
            jax.ShapeDtypeStruct(own.shape, F32),
            jax.ShapeDtypeStruct(own.shape, BF16),
        ],
        name="project",
    )(base, mixed, mine, other, change, own, gate_a, shift_m, scale_m)


def feed_part(rows_ref, own_ref, pair_ref, up_ref, down_ref, so_far):
    count = own_ref.shape[0]

    @pl.when(pl.program_id(0) == 0)
    def _():
        rows_ref[:count] = own_ref[...]
        rows_ref[count:] = pair_ref[...]

    hidden = jax.nn.gelu(dot(rows_ref[...], up_ref[...]), approximate=True).astype(BF16)
    return so_far() + dot_t(hidden, down_ref[...])


def feed_first_body(own_ref, pair_ref, up_ref, down_ref, sum_ref, rows_ref):
    @pl.when(pl.program_id(0) == 0)
    def _():
        sum_ref[...] = jnp.zeros(sum_ref.shape, F32)

    sum_ref[...] = feed_part(rows_ref, own_ref, pair_ref, up_ref, down_ref, lambda: sum_ref[...])


def feed_second_body(own_ref, pair_ref, up_ref, down_ref, before_ref, keep_ref, send_ref, rows_ref, sum_ref):
    count = own_ref.shape[0]

    @pl.when(pl.program_id(0) == 0)
    def _():
        sum_ref[...] = before_ref[...]

    sum_ref[...] = feed_part(rows_ref, own_ref, pair_ref, up_ref, down_ref, lambda: sum_ref[...])

    @pl.when(pl.program_id(0) == pl.num_programs(0) - 1)
    def _():
        keep_ref[...] = sum_ref[:count]
        send_ref[...] = sum_ref[count:].astype(BF16)


def feed_first(own, pair, weights):
    count, width = own.shape
    steps = 3
    up = pl.BlockSpec((width, width // steps), lambda i: (0, steps + i))
    down = pl.BlockSpec((width, width // steps), lambda i: (0, i))
    return pl.pallas_call(
        feed_first_body,
        grid=(steps,),
        in_specs=[whole(own.shape), whole(own.shape), up, down],
        out_specs=whole((2 * count, width)),
        out_shape=jax.ShapeDtypeStruct((2 * count, width), F32),
        scratch_shapes=[pltpu.VMEM((2 * count, width), BF16)],
        name="feed_first",
    )(own, pair, weights, weights)


def feed_second(own, pair, weights, before):
    count, width = own.shape
    steps = 3
    up = pl.BlockSpec((width, width // steps), lambda i: (0, steps + i))
    down = pl.BlockSpec((width, width // steps), lambda i: (0, i))
    return pl.pallas_call(
        feed_second_body,
        grid=(steps,),
        in_specs=[whole(own.shape), whole(own.shape), up, down, whole(before.shape)],
        out_specs=[whole(own.shape), whole(own.shape)],
        out_shape=[
            jax.ShapeDtypeStruct(own.shape, F32),
            jax.ShapeDtypeStruct(own.shape, BF16),
        ],
        scratch_shapes=[pltpu.VMEM((2 * count, width), BF16), pltpu.VMEM((2 * count, width), F32)],
        name="feed_second",
    )(own, pair, weights, weights, before)


def finish_body(scale_by_ref, keep_ref, recv_ref, first_ref, gate_ref, shift_ref, scale_ref, out_w_ref, out_ref):
    share = first_ref.shape[1]
    noise = []
    for i in range(2):
        part = slice(i * share, (i + 1) * share)
        mlp = keep_ref[part] + recv_ref[part].astype(F32)
        total = first_ref[i] + gate_ref[i] * mlp
        fin = (layer_norm(total) * (1.0 + scale_ref[i]) + shift_ref[i]).astype(BF16)
        noise.append(dot(fin, out_w_ref[...]))
    out_ref[...] = noise[1] + scale_by_ref[0] * (noise[0] - noise[1])


def finish(guidance, keep, recv, first_sum, gate_m, shift_f, scale_f, out_local):
    _, share, width = first_sum.shape
    vector = whole((2, 1, width))
    return pl.pallas_call(
        finish_body,
        grid_spec=pltpu.PrefetchScalarGridSpec(
            num_scalar_prefetch=1,
            grid=(1,),
            in_specs=[
                whole(keep.shape),
                whole(recv.shape),
                whole(first_sum.shape),
                vector,
                vector,
                vector,
                whole(out_local.shape),
            ],
            out_specs=whole((share, out_local.shape[1])),
        ),
        out_shape=jax.ShapeDtypeStruct((share, out_local.shape[1]), F32),
        name="finish",
    )(guidance, keep, recv, first_sum, gate_m, shift_f, scale_f, out_local)


def on_device(
    x_arrive,
    cond_first,
    labels,
    step_ids,
    guidance,
    time_table,
    class_table,
    ada_weight,
    final_ada,
    qkv_weight,
    proj_weight,
    fc1_weight,
    fc2_weight,
    out_weight,
):
    tokens = x_arrive.shape[1]
    width = x_arrive.shape[2]
    rows = qkv_weight.shape[1]
    quarter = qkv_weight.shape[2]
    core = lax.axis_index("group")
    column = lax.axis_index("dp_1")
    high = lax.axis_index("dp_2")
    place = lax.axis_index("mp")
    n_y, n_x, n_z = (lax.axis_size(axis) for axis in DP)
    n_mp = lax.axis_size("mp")
    half = quarter // 2

    time_part = jnp.take(time_table, step_ids, axis=0).astype(F32)
    class_part = jnp.take(class_table, labels, axis=0).astype(F32)
    null_part = class_table[CLASSES].astype(F32)[None, :]
    acts = jax.nn.silu(jnp.concatenate([time_part + class_part, time_part + null_part])).astype(BF16)
    every_act = to_everyone(acts, DP).reshape(-1, acts.shape[1])

    qkv_own = jnp.where(core == 0, qkv_weight[:, :, :half], qkv_weight[:, :, half:])
    qkv_own = qkv_own.transpose(1, 0, 2).reshape(rows, 3 * half)

    shards = jnp.concatenate([fc2_weight.T, fc1_weight, proj_weight.T, qkv_own], axis=1)
    shards = by_height(shards, swap(shards, "dp_2", 1), high)
    qkv_block = shards[:, 2 * width + quarter :]

    def fetch(x, along):
        pairs = [(c * n_mp + m, c * n_mp + (m ^ (2 * c) ^ along)) for c in range(2) for m in range(n_mp)]
        return lax.ppermute(x, ("group", "mp"), pairs)

    feed = fetch(shards[:, : 2 * width + quarter], 0)
    proj_beside = fetch(shards[:, 2 * width : 2 * width + quarter], 1)
    part_a = lanes_full(jnp.concatenate([qkv_block, feed[:, 2 * width :], proj_beside], axis=1))
    part_a, every_act = lax.optimization_barrier((part_a, every_act))
    part_a = gather_y(part_a)
    part_a, every_act = lax.optimization_barrier((part_a, every_act))
    part_a = gather_x(part_a)
    other_a = swap(part_a, "group", 1)

    feed = lax.all_gather(feed[:, : 2 * width], "dp_0", axis=0, tiled=True)
    feed = lax.all_gather(feed, "dp_1", axis=0, tiled=True)
    other_feed = swap(feed, "group", 1)

    mod_part = dot(every_act, ada_weight).astype(BF16)
    mod_part = lax.all_to_all(mod_part, DP, split_axis=0, concat_axis=1, tiled=True)
    final_part = dot(acts, final_ada).astype(BF16)
    mod_parts = to_everyone(jnp.concatenate([mod_part, final_part], axis=1), "mp")

    spot = lax.broadcasted_iota(jnp.int32, (1, width), 1)
    per_x = n_y * n_z * rows
    per_y = n_z * rows
    block = spot // per_x
    inside = spot % per_x
    offset = jnp.where(block == 1, n_x - 1, jnp.where(block == 2, 1, jnp.where(block == 3, 2, 0)))

    from_x = (column + offset) % n_x
    final = (inside // per_y * n_x + from_x) * per_y + inside % per_y
    near_order = (lax.broadcasted_iota(jnp.int32, (width, width), 0) == final).astype(BF16)
    natural = (inside // per_y * n_x + block) * per_y + inside % per_y
    order = (lax.broadcasted_iota(jnp.int32, (width, width), 0) == natural).astype(BF16)
    change = (final.reshape(width, 1) == natural).astype(BF16)

    first = cond_first[0] == 1
    cond_rows = jnp.where(first, x_arrive[0], x_arrive[1])
    uncond_rows = jnp.where(first, x_arrive[1], x_arrive[0])
    arrived = jnp.stack([cond_rows, uncond_rows])
    share = tokens // n_mp
    own = lax.dynamic_slice_in_dim(arrived, place * share, share, 1)
    own = dot(own.reshape(-1, width), order).astype(BF16).reshape(2, share, width)
    images = dot(arrived.reshape(-1, width), near_order).astype(BF16)
    images = images.reshape(2, tokens, width)
    out_local = lax.dot_general(
        order, out_weight, (((0,), (0,)), ((), ())), preferred_element_type=F32
    ).astype(BF16)
    mod_parts = mod_parts.reshape(n_mp * 2, -1, width)

    def mods_in(pieces, by):
        count = pieces.shape[1]
        values = dot(pieces.reshape(-1, width), by).reshape(n_mp, 2, count, 1, width)
        values = jnp.sum(values, axis=0)
        return [values[:, i] for i in range(count)]

    shift_a, scale_a = mods_in(mod_parts[:, :2], near_order)
    gate_a, shift_m, scale_m, gate_m, shift_f, scale_f = mods_in(mod_parts[:, 2:], order)

    cores = core.reshape(1).astype(jnp.int32)
    mixed = attention(cores, images, shift_a, scale_a, part_a, other_a, n_mp, quarter)
    mixed = lax.all_to_all(mixed, "mp", 0, 0, tiled=True)
    base = (place ^ (2 * core)).reshape(1).astype(jnp.int32)
    first_sum, hidden_two = project(base, mixed, part_a, other_a, change, own, gate_a, shift_m, scale_m)
    hidden_two = hidden_two.reshape(2 * share, width)
    pair = swap(hidden_two, "mp", 1)
    before = feed_first(hidden_two, pair, feed)
    keep, send = feed_second(hidden_two, pair, other_feed, before)
    recv = swap(send, "mp", 1)
    guided = finish(guidance, keep, recv, first_sum, gate_m, shift_f, scale_f, out_local)
    return guided.reshape(1, share * out_weight.shape[1])


def solution(mesh):
    torus = Mesh(
        mesh.devices.reshape(mesh.shape["group"], 8, 4, 2, mesh.shape["mp"]),
        ("group", "dp_0", "dp_1", "dp_2", "mp"),
    )
    placed = (
        P(GROUP_DP, None, None),
        P(GROUP_DP),
        P(GROUP_DP),
        P(GROUP_DP),
        P(),
        P(None, "mp"),
        P(None, "mp"),
        P("mp", DP),
        P("mp", None),
        P(None, DP, "mp"),
        P("mp", DP),
        P(DP, "mp"),
        P("mp", DP),
        P(),
    )
    return jax.shard_map(on_device, mesh=torus, in_specs=placed, out_specs=P(GROUP_DP, "mp"), check_vma=False)
```

```python
import jax
import jax.numpy as jnp
from jax import lax
from jax.experimental import pallas as pl
from jax.experimental.pallas import tpu as pltpu
from jax.sharding import Mesh
from jax.sharding import PartitionSpec as P

CLASSES = 1000
DP = ("dp_0", "dp_1", "dp_2")
GROUP_DP = ("group", "dp_0", "dp_1", "dp_2")
BF16 = jnp.bfloat16
F32 = jnp.float32


def to_everyone(x, axis):
    size = lax.axis_size(axis)
    return lax.all_to_all(jnp.broadcast_to(x[None], (size, *x.shape)), axis, 0, 0, tiled=True)


def shift(x, axis, step):
    size = lax.axis_size(axis)
    return lax.ppermute(x, axis, [(i, (i + step) % size) for i in range(size)])


def swap(x, axis, bit):
    size = lax.axis_size(axis)
    return lax.ppermute(x, axis, [(i, i ^ bit) for i in range(size)])


def gather_x(block):
    half = block.shape[0] // 2
    left = shift(block, "dp_1", 1)
    right = shift(block, "dp_1", -1)
    far_top = shift(left[:half], "dp_1", 1)
    far_bottom = shift(right[half:], "dp_1", -1)
    return jnp.concatenate([block, left, right, far_top, far_bottom], axis=0)


def by_height(own, other, high):
    own_low = high == 0
    return jnp.concatenate([jnp.where(own_low, own, other), jnp.where(own_low, other, own)])


def lanes_full(x):
    return jnp.pad(x, ((0, 0), (0, -x.shape[1] % 128)))


def layer_norm(values):
    mean = jnp.mean(values, axis=-1, keepdims=True)
    centred = values - mean
    spread = jnp.mean(centred * centred, axis=-1, keepdims=True)
    return centred * lax.rsqrt(spread + 1e-06)


def dot(a, b):
    return jnp.dot(a, b, preferred_element_type=F32)


def dot_t(a, b):
    return lax.dot_general(a, b, (((1,), (1,)), ((), ())), preferred_element_type=F32)


def whole(shape):
    return pl.BlockSpec(shape, lambda *_: (0,) * len(shape))


def attention_body(core_ref, x_ref, shift_ref, scale_ref, mine_ref, other_ref, out_ref):
    images, tokens, _ = x_ref.shape
    pieces, quarter, _ = out_ref.shape
    head_dim = quarter // 4
    share = tokens // pieces
    scale = head_dim ** (-0.5)
    low = core_ref[0] == 0
    for image in range(images):
        x = x_ref[image].astype(F32)
        hidden = (layer_norm(x) * (1.0 + scale_ref[image]) + shift_ref[image]).astype(BF16)
        sides = []
        for ref in (mine_ref, other_ref):
            qkv = dot(hidden, ref[:, : 6 * head_dim]).astype(BF16)
            heads = []
            for head in range(2):
                at = head * head_dim
                query = qkv[:, at : at + head_dim]
                keys = qkv[:, 2 * head_dim + at : 3 * head_dim + at]
                values = qkv[:, 4 * head_dim + at : 5 * head_dim + at]
                scores = dot_t(query, keys) * scale
                top = jnp.max(scores, axis=-1, keepdims=True)
                weights = jnp.exp(scores - top)
                total = jnp.sum(weights, axis=-1, keepdims=True)
                probs = (weights * (1.0 / total)).astype(BF16)
                mixed = lax.dot_general(
                    values, probs, (((0,), (1,)), ((), ())), preferred_element_type=F32
                )
                heads.append(mixed.astype(BF16))
            sides.append(jnp.concatenate(heads, axis=0))
        first = jnp.where(low, sides[0], sides[1])
        second = jnp.where(low, sides[1], sides[0])
        mixed = jnp.concatenate([first, second], axis=0)
        for piece in range(pieces):
            part = mixed[:, piece * share : (piece + 1) * share]
            out_ref[piece, :, image * share : (image + 1) * share] = part


def attention(core, x, shift_a, scale_a, mine, other, n_mp, quarter):
    images, tokens, width = x.shape
    vector = whole((images, 1, width))
    out_shape = (n_mp, quarter, images * tokens // n_mp)
    return pl.pallas_call(
        attention_body,
        grid_spec=pltpu.PrefetchScalarGridSpec(
            num_scalar_prefetch=1,
            grid=(1,),
            in_specs=[whole(x.shape), vector, vector, whole(mine.shape), whole(other.shape)],
            out_specs=whole(out_shape),
        ),
        out_shape=jax.ShapeDtypeStruct(out_shape, BF16),
        name="attention",
    )(core, x, shift_a, scale_a, mine, other)


def project_body(base_ref, mixed_ref, mine_ref, other_ref, change_ref, own_ref, gate_ref, shift_ref, scale_ref,
                 sum_ref, hidden_ref, rows_ref):
    quarter = mixed_ref.shape[1]
    start = 3 * quarter // 2
    lead = start % 128
    base = base_ref[0]
    rows_ref[...] = jnp.zeros(rows_ref.shape, BF16)
    for i in range(4):
        at = lead + i % 2 * quarter
        rows_ref[i // 2, at : at + quarter] = mixed_ref[base ^ i]
    both = (((0,), (1,)), ((), ()))
    attn = lax.dot_general(
        rows_ref[0], mine_ref[:, start - lead :], both, preferred_element_type=F32
    ) + lax.dot_general(
        rows_ref[1], other_ref[:, start - lead :], both, preferred_element_type=F32
    )
    attn = dot(attn.astype(BF16), change_ref[...])
    share = own_ref.shape[1]
    for i in range(2):
        total = own_ref[i].astype(F32) + gate_ref[i] * attn[i * share : (i + 1) * share]
        sum_ref[i] = total
        hidden_ref[i] = (layer_norm(total) * (1.0 + scale_ref[i]) + shift_ref[i]).astype(BF16)


def project(base, mixed, mine, other, change, own, gate_a, shift_m, scale_m):
    _, share, width = own.shape
    vector = whole((2, 1, width))
    start = 3 * mixed.shape[1] // 2
    depth = mine.shape[1] - start // 128 * 128
    return pl.pallas_call(
        project_body,
        grid_spec=pltpu.PrefetchScalarGridSpec(
            num_scalar_prefetch=1,
            grid=(1,),
            in_specs=[
                whole(mixed.shape),
                whole(mine.shape),
                whole(other.shape),
                whole(change.shape),
                whole(own.shape),
                vector,
                vector,
                vector,
            ],
            out_specs=[whole(own.shape), whole(own.shape)],
            scratch_shapes=[pltpu.VMEM((2, depth, 2 * share), BF16)],
        ),
        out_shape=[
            jax.ShapeDtypeStruct(own.shape, F32),
            jax.ShapeDtypeStruct(own.shape, BF16),
        ],
        name="project",
    )(base, mixed, mine, other, change, own, gate_a, shift_m, scale_m)


def feed_part(rows_ref, own_ref, pair_ref, up_ref, down_ref, so_far):
    count = own_ref.shape[0]

    @pl.when(pl.program_id(0) == 0)
    def _():
        rows_ref[:count] = own_ref[...]
        rows_ref[count:] = pair_ref[...]

    hidden = jax.nn.gelu(dot(rows_ref[...], up_ref[...]), approximate=True).astype(BF16)
    return so_far() + dot_t(hidden, down_ref[...])


def feed_first_body(own_ref, pair_ref, up_ref, down_ref, sum_ref, rows_ref):
    @pl.when(pl.program_id(0) == 0)
    def _():
        sum_ref[...] = jnp.zeros(sum_ref.shape, F32)

    sum_ref[...] = feed_part(rows_ref, own_ref, pair_ref, up_ref, down_ref, lambda: sum_ref[...])


def feed_second_body(own_ref, pair_ref, up_ref, down_ref, before_ref, keep_ref, send_ref, rows_ref, sum_ref):
    count = own_ref.shape[0]

    @pl.when(pl.program_id(0) == 0)
    def _():
        sum_ref[...] = before_ref[...]

    sum_ref[...] = feed_part(rows_ref, own_ref, pair_ref, up_ref, down_ref, lambda: sum_ref[...])

    @pl.when(pl.program_id(0) == pl.num_programs(0) - 1)
    def _():
        keep_ref[...] = sum_ref[:count]
        send_ref[...] = sum_ref[count:].astype(BF16)


def feed_first(own, pair, weights):
    count, width = own.shape
    steps = 3
    up = pl.BlockSpec((width, width // steps), lambda i: (0, steps + i))
    down = pl.BlockSpec((width, width // steps), lambda i: (0, i))
    return pl.pallas_call(
        feed_first_body,
        grid=(steps,),
        in_specs=[whole(own.shape), whole(own.shape), up, down],
        out_specs=whole((2 * count, width)),
        out_shape=jax.ShapeDtypeStruct((2 * count, width), F32),
        scratch_shapes=[pltpu.VMEM((2 * count, width), BF16)],
        name="feed_first",
    )(own, pair, weights, weights)


def feed_second(own, pair, weights, before):
    count, width = own.shape
    steps = 3
    up = pl.BlockSpec((width, width // steps), lambda i: (0, steps + i))
    down = pl.BlockSpec((width, width // steps), lambda i: (0, i))
    return pl.pallas_call(
        feed_second_body,
        grid=(steps,),
        in_specs=[whole(own.shape), whole(own.shape), up, down, whole(before.shape)],
        out_specs=[whole(own.shape), whole(own.shape)],
        out_shape=[
            jax.ShapeDtypeStruct(own.shape, F32),
            jax.ShapeDtypeStruct(own.shape, BF16),
        ],
        scratch_shapes=[pltpu.VMEM((2 * count, width), BF16), pltpu.VMEM((2 * count, width), F32)],
        name="feed_second",
    )(own, pair, weights, weights, before)


def finish_body(scale_by_ref, keep_ref, recv_ref, first_ref, gate_ref, shift_ref, scale_ref, out_w_ref, out_ref):
    share = first_ref.shape[1]
    noise = []
    for i in range(2):
        part = slice(i * share, (i + 1) * share)
        mlp = keep_ref[part] + recv_ref[part].astype(F32)
        total = first_ref[i] + gate_ref[i] * mlp
        fin = (layer_norm(total) * (1.0 + scale_ref[i]) + shift_ref[i]).astype(BF16)
        noise.append(dot(fin, out_w_ref[...]))
    guided = noise[1] + scale_by_ref[0] * (noise[0] - noise[1])
    outs = guided.shape[1]
    wide = jnp.concatenate([guided] * (128 // outs), axis=1)
    wide = jnp.concatenate([wide] * (share * outs // 128), axis=1)
    token = lax.broadcasted_iota(jnp.int32, wide.shape, 0)
    mine = lax.broadcasted_iota(jnp.int32, wide.shape, 1) // outs == token
    out_ref[...] = jnp.sum(jnp.where(mine, wide, 0.0), axis=0, keepdims=True)


def finish(guidance, keep, recv, first_sum, gate_m, shift_f, scale_f, out_local):
    _, share, width = first_sum.shape
    vector = whole((2, 1, width))
    return pl.pallas_call(
        finish_body,
        grid_spec=pltpu.PrefetchScalarGridSpec(
            num_scalar_prefetch=1,
            grid=(1,),
            in_specs=[
                whole(keep.shape),
                whole(recv.shape),
                whole(first_sum.shape),
                vector,
                vector,
                vector,
                whole(out_local.shape),
            ],
            out_specs=whole((1, share * out_local.shape[1])),
        ),
        out_shape=jax.ShapeDtypeStruct((1, share * out_local.shape[1]), F32),
        name="finish",
    )(guidance, keep, recv, first_sum, gate_m, shift_f, scale_f, out_local)


def on_device(
    x_arrive,
    cond_first,
    labels,
    step_ids,
    guidance,
    time_table,
    class_table,
    ada_weight,
    final_ada,
    qkv_weight,
    proj_weight,
    fc1_weight,
    fc2_weight,
    out_weight,
):
    tokens = x_arrive.shape[1]
    width = x_arrive.shape[2]
    rows = qkv_weight.shape[1]
    quarter = qkv_weight.shape[2]
    core = lax.axis_index("group")
    column = lax.axis_index("dp_1")
    high = lax.axis_index("dp_2")
    place = lax.axis_index("mp")
    n_y, n_x, n_z = (lax.axis_size(axis) for axis in DP)
    n_mp = lax.axis_size("mp")
    half = quarter // 2

    time_part = jnp.take(time_table, step_ids, axis=0).astype(F32)
    class_part = jnp.take(class_table, labels, axis=0).astype(F32)
    null_part = class_table[CLASSES].astype(F32)[None, :]
    acts = jax.nn.silu(jnp.concatenate([time_part + class_part, time_part + null_part])).astype(BF16)
    every_act = to_everyone(acts, DP).reshape(-1, acts.shape[1])

    qkv_own = jnp.where(core == 0, qkv_weight[:, :, :half], qkv_weight[:, :, half:])
    qkv_own = qkv_own.transpose(1, 0, 2).reshape(rows, 3 * half)

    shards = jnp.concatenate([fc2_weight.T, fc1_weight, proj_weight.T, qkv_own], axis=1)
    shards = by_height(shards, swap(shards, "dp_2", 1), high)
    qkv_block = shards[:, 2 * width + quarter :]

    def fetch(x, along):
        pairs = [(c * n_mp + m, c * n_mp + (m ^ (2 * c) ^ along)) for c in range(2) for m in range(n_mp)]
        return lax.ppermute(x, ("group", "mp"), pairs)

    feed = fetch(shards[:, : 2 * width + quarter], 0)
    proj_beside = fetch(shards[:, 2 * width : 2 * width + quarter], 1)
    part_a = lanes_full(jnp.concatenate([qkv_block, feed[:, 2 * width :], proj_beside], axis=1))

    mod_part = dot(every_act, ada_weight).astype(BF16)
    pad = -mod_part.shape[1] % 128
    columns = mod_part.shape[1]
    mod_part = jnp.pad(mod_part, ((0, 0), (0, pad))).reshape(n_y, n_x * n_z, 2, columns + pad)
    mod_part = mod_part.transpose(1, 0, 2, 3)
    mod_part = lax.all_to_all(mod_part, DP[1:], 0, 0, tiled=True)
    mod_part = mod_part.transpose(1, 2, 0, 3).reshape(n_y, -1, part_a.shape[1])
    block_rows = part_a.shape[0]
    part_a = jnp.broadcast_to(part_a[None], (n_y, *part_a.shape))
    part_a = jnp.concatenate([part_a, mod_part], axis=1)
    part_a = lax.all_to_all(part_a, "dp_0", 0, 0, tiled=True)
    mod_part = part_a[:, block_rows:].reshape(n_y, 2, n_x * n_z, columns + pad)
    mod_part = mod_part[..., :columns].transpose(1, 0, 2, 3).reshape(2, -1)
    part_a = part_a[:, :block_rows].reshape(n_y * block_rows, -1)
    part_a = gather_x(part_a)
    other_a = swap(part_a, "group", 1)

    feed = lax.all_gather(feed[:, : 2 * width], "dp_0", axis=0, tiled=True)
    feed = lax.all_gather(feed, "dp_1", axis=0, tiled=True)
    other_feed = swap(feed, "group", 1)

    final_part = dot(acts, final_ada).astype(BF16)
    mod_parts = to_everyone(jnp.concatenate([mod_part, final_part], axis=1), "mp")

    spot = lax.broadcasted_iota(jnp.int32, (1, width), 1)
    per_x = n_y * n_z * rows
    per_y = n_z * rows
    block = spot // per_x
    inside = spot % per_x
    offset = jnp.where(block == 1, n_x - 1, jnp.where(block == 2, 1, jnp.where(block == 3, 2, 0)))

    from_x = (column + offset) % n_x
    final = (inside // per_y * n_x + from_x) * per_y + inside % per_y
    near_order = (lax.broadcasted_iota(jnp.int32, (width, width), 0) == final).astype(BF16)
    natural = (inside // per_y * n_x + block) * per_y + inside % per_y
    order = (lax.broadcasted_iota(jnp.int32, (width, width), 0) == natural).astype(BF16)
    change = (final.reshape(width, 1) == natural).astype(BF16)

    first = cond_first[0] == 1
    cond_rows = jnp.where(first, x_arrive[0], x_arrive[1])
    uncond_rows = jnp.where(first, x_arrive[1], x_arrive[0])
    arrived = jnp.stack([cond_rows, uncond_rows])
    share = tokens // n_mp
    own = lax.dynamic_slice_in_dim(arrived, place * share, share, 1)
    own = dot(own.reshape(-1, width), order).astype(BF16).reshape(2, share, width)
    images = dot(arrived.reshape(-1, width), near_order).astype(BF16)
    images = images.reshape(2, tokens, width)
    out_local = lax.dot_general(
        order, out_weight, (((0,), (0,)), ((), ())), preferred_element_type=F32
    ).astype(BF16)
    mod_parts = mod_parts.reshape(n_mp * 2, -1, width)

    def mods_in(pieces, by):
        count = pieces.shape[1]
        values = dot(pieces.reshape(-1, width), by).reshape(n_mp, 2, count, 1, width)
        values = jnp.sum(values, axis=0)
        return [values[:, i] for i in range(count)]

    shift_a, scale_a = mods_in(mod_parts[:, :2], near_order)
    gate_a, shift_m, scale_m, gate_m, shift_f, scale_f = mods_in(mod_parts[:, 2:], order)

    cores = core.reshape(1).astype(jnp.int32)
    mixed = attention(cores, images, shift_a, scale_a, part_a, other_a, n_mp, quarter)
    mixed = lax.all_to_all(mixed, "mp", 0, 0, tiled=True)
    base = (place ^ (2 * core)).reshape(1).astype(jnp.int32)
    first_sum, hidden_two = project(base, mixed, part_a, other_a, change, own, gate_a, shift_m, scale_m)
    hidden_two = hidden_two.reshape(2 * share, width)
    pair = swap(hidden_two, "mp", 1)
    before = feed_first(hidden_two, pair, feed)
    keep, send = feed_second(hidden_two, pair, other_feed, before)
    recv = swap(send, "mp", 1)
    return finish(guidance, keep, recv, first_sum, gate_m, shift_f, scale_f, out_local)


def solution(mesh):
    torus = Mesh(
        mesh.devices.reshape(mesh.shape["group"], 8, 4, 2, mesh.shape["mp"]),
        ("group", "dp_0", "dp_1", "dp_2", "mp"),
    )
    placed = (
        P(GROUP_DP, None, None),
        P(GROUP_DP),
        P(GROUP_DP),
        P(GROUP_DP),
        P(),
        P(None, "mp"),
        P(None, "mp"),
        P("mp", DP),
        P("mp", None),
        P(None, DP, "mp"),
        P("mp", DP),
        P(DP, "mp"),
        P("mp", DP),
        P(),
    )
    return jax.shard_map(
        on_device, mesh=torus, in_specs=placed, out_specs=P(GROUP_DP, "mp"), check_vma=False
    )
```

```python
import jax
import jax.numpy as jnp
from jax import lax
from jax.experimental import pallas as pl
from jax.experimental.pallas import tpu as pltpu
from jax.sharding import Mesh
from jax.sharding import PartitionSpec as P

CLASSES = 1000
GATHER_FLOOR = 1 << 20
DP = ("dp_0", "dp_1", "dp_2")
GROUP_DP = ("group", "dp_0", "dp_1", "dp_2")
BF16 = jnp.bfloat16
F32 = jnp.float32


def to_everyone(x, axis):
    size = lax.axis_size(axis)
    return lax.all_to_all(jnp.broadcast_to(x[None], (size, *x.shape)), axis, 0, 0, tiled=True)


def shift(x, axis, step):
    size = lax.axis_size(axis)
    return lax.ppermute(x, axis, [(i, (i + step) % size) for i in range(size)])


def swap(x, axis, bit):
    size = lax.axis_size(axis)
    return lax.ppermute(x, axis, [(i, i ^ bit) for i in range(size)])


def gather_y(block):
    pieces = to_everyone(block, "dp_0")
    return pieces.reshape(pieces.shape[0] * pieces.shape[1], pieces.shape[2])


def gather_x(block):
    half = block.shape[0] // 2
    left = shift(block, "dp_1", 1)
    right = shift(block, "dp_1", -1)
    far_top = shift(left[:half], "dp_1", 1)
    far_bottom = shift(right[half:], "dp_1", -1)
    return jnp.concatenate([block, left, right, far_top, far_bottom], axis=0)


def by_height(own, other, high):
    own_low = high == 0
    return jnp.concatenate([jnp.where(own_low, own, other), jnp.where(own_low, other, own)])


def lanes_full(x):
    return jnp.pad(x, ((0, 0), (0, -x.shape[1] % 128)))


def layer_norm(values):
    mean = jnp.mean(values, axis=-1, keepdims=True)
    centred = values - mean
    spread = jnp.mean(centred * centred, axis=-1, keepdims=True)
    return centred * lax.rsqrt(spread + 1e-06)


def dot(a, b):
    return jnp.dot(a, b, preferred_element_type=F32)


def dot_t(a, b):
    return lax.dot_general(a, b, (((1,), (1,)), ((), ())), preferred_element_type=F32)


def whole(shape):
    return pl.BlockSpec(shape, lambda *_: (0,) * len(shape))


def attention_body(core_ref, x_ref, shift_ref, scale_ref, mine_ref, other_ref, out_ref):
    images, tokens, _ = x_ref.shape
    pieces, quarter, _ = out_ref.shape
    head_dim = quarter // 4
    share = tokens // pieces
    scale = head_dim ** (-0.5)
    low = core_ref[0] == 0
    for image in range(images):
        x = x_ref[image].astype(F32)
        hidden = (layer_norm(x) * (1.0 + scale_ref[image]) + shift_ref[image]).astype(BF16)
        sides = []
        for ref in (mine_ref, other_ref):
            qkv = dot(hidden, ref[:, : 6 * head_dim]).astype(BF16)
            heads = []
            for head in range(2):
                at = head * head_dim
                query = qkv[:, at : at + head_dim]
                keys = qkv[:, 2 * head_dim + at : 3 * head_dim + at]
                values = qkv[:, 4 * head_dim + at : 5 * head_dim + at]
                scores = dot_t(query, keys) * scale
                top = jnp.max(scores, axis=-1, keepdims=True)
                weights = jnp.exp(scores - top)
                total = jnp.sum(weights, axis=-1, keepdims=True)
                probs = (weights * (1.0 / total)).astype(BF16)
                mixed = lax.dot_general(
                    values, probs, (((0,), (1,)), ((), ())), preferred_element_type=F32
                )
                heads.append(mixed.astype(BF16))
            sides.append(jnp.concatenate(heads, axis=0))
        first = jnp.where(low, sides[0], sides[1])
        second = jnp.where(low, sides[1], sides[0])
        mixed = jnp.concatenate([first, second], axis=0)
        for piece in range(pieces):
            part = mixed[:, piece * share : (piece + 1) * share]
            out_ref[piece, :, image * share : (image + 1) * share] = part


def attention(core, x, shift_a, scale_a, mine, other, n_mp, quarter):
    images, tokens, width = x.shape
    vector = whole((images, 1, width))
    out_shape = (n_mp, quarter, images * tokens // n_mp)
    return pl.pallas_call(
        attention_body,
        grid_spec=pltpu.PrefetchScalarGridSpec(
            num_scalar_prefetch=1,
            grid=(1,),
            in_specs=[whole(x.shape), vector, vector, whole(mine.shape), whole(other.shape)],
            out_specs=whole(out_shape),
        ),
        out_shape=jax.ShapeDtypeStruct(out_shape, BF16),
        name="attention",
    )(core, x, shift_a, scale_a, mine, other)


def project_body(base_ref, mixed_ref, mine_ref, other_ref, change_ref, own_ref, gate_ref, shift_ref, scale_ref,
                 sum_ref, hidden_ref, rows_ref):
    quarter = mixed_ref.shape[1]
    start = 3 * quarter // 2
    lead = start % 128
    base = base_ref[0]
    rows_ref[...] = jnp.zeros(rows_ref.shape, BF16)
    for i in range(4):
        at = lead + i % 2 * quarter
        rows_ref[i // 2, at : at + quarter] = mixed_ref[base ^ i]
    both = (((0,), (1,)), ((), ()))
    attn = lax.dot_general(
        rows_ref[0], mine_ref[:, start - lead :], both, preferred_element_type=F32
    ) + lax.dot_general(
        rows_ref[1], other_ref[:, start - lead :], both, preferred_element_type=F32
    )
    attn = dot(attn.astype(BF16), change_ref[...])
    share = own_ref.shape[1]
    for i in range(2):
        total = own_ref[i].astype(F32) + gate_ref[i] * attn[i * share : (i + 1) * share]
        sum_ref[i] = total
        hidden_ref[i] = (layer_norm(total) * (1.0 + scale_ref[i]) + shift_ref[i]).astype(BF16)


def project(base, mixed, mine, other, change, own, gate_a, shift_m, scale_m):
    _, share, width = own.shape
    vector = whole((2, 1, width))
    start = 3 * mixed.shape[1] // 2
    depth = mine.shape[1] - start // 128 * 128
    return pl.pallas_call(
        project_body,
        grid_spec=pltpu.PrefetchScalarGridSpec(
            num_scalar_prefetch=1,
            grid=(1,),
            in_specs=[
                whole(mixed.shape),
                whole(mine.shape),
                whole(other.shape),
                whole(change.shape),
                whole(own.shape),
                vector,
                vector,
                vector,
            ],
            out_specs=[whole(own.shape), whole(own.shape)],
            scratch_shapes=[pltpu.VMEM((2, depth, 2 * share), BF16)],
        ),
        out_shape=[
            jax.ShapeDtypeStruct(own.shape, F32),
            jax.ShapeDtypeStruct(own.shape, BF16),
        ],
        name="project",
    )(base, mixed, mine, other, change, own, gate_a, shift_m, scale_m)


def feed_part(rows_ref, own_ref, pair_ref, up_ref, down_ref, so_far):
    count = own_ref.shape[0]

    @pl.when(pl.program_id(0) == 0)
    def _():
        rows_ref[:count] = own_ref[...]
        rows_ref[count:] = pair_ref[...]

    hidden = jax.nn.gelu(dot(rows_ref[...], up_ref[...]), approximate=True).astype(BF16)
    return so_far() + dot_t(hidden, down_ref[...])


def feed_first_body(own_ref, pair_ref, up_ref, down_ref, sum_ref, rows_ref):
    @pl.when(pl.program_id(0) == 0)
    def _():
        sum_ref[...] = jnp.zeros(sum_ref.shape, F32)

    sum_ref[...] = feed_part(rows_ref, own_ref, pair_ref, up_ref, down_ref, lambda: sum_ref[...])


def feed_second_body(own_ref, pair_ref, up_ref, down_ref, before_ref, keep_ref, send_ref, rows_ref, sum_ref):
    count = own_ref.shape[0]

    @pl.when(pl.program_id(0) == 0)
    def _():
        sum_ref[...] = before_ref[...]

    sum_ref[...] = feed_part(rows_ref, own_ref, pair_ref, up_ref, down_ref, lambda: sum_ref[...])

    @pl.when(pl.program_id(0) == pl.num_programs(0) - 1)
    def _():
        keep_ref[...] = sum_ref[:count]
        send_ref[...] = sum_ref[count:].astype(BF16)


def feed_first(own, pair, weights):
    count, width = own.shape
    steps = 3
    up = pl.BlockSpec((width, width // steps), lambda i: (0, steps + i))
    down = pl.BlockSpec((width, width // steps), lambda i: (0, i))
    return pl.pallas_call(
        feed_first_body,
        grid=(steps,),
        in_specs=[whole(own.shape), whole(own.shape), up, down],
        out_specs=whole((2 * count, width)),
        out_shape=jax.ShapeDtypeStruct((2 * count, width), F32),
        scratch_shapes=[pltpu.VMEM((2 * count, width), BF16)],
        name="feed_first",
    )(own, pair, weights, weights)


def feed_second(own, pair, weights, before):
    count, width = own.shape
    steps = 3
    up = pl.BlockSpec((width, width // steps), lambda i: (0, steps + i))
    down = pl.BlockSpec((width, width // steps), lambda i: (0, i))
    return pl.pallas_call(
        feed_second_body,
        grid=(steps,),
        in_specs=[whole(own.shape), whole(own.shape), up, down, whole(before.shape)],
        out_specs=[whole(own.shape), whole(own.shape)],
        out_shape=[
            jax.ShapeDtypeStruct(own.shape, F32),
            jax.ShapeDtypeStruct(own.shape, BF16),
        ],
        scratch_shapes=[pltpu.VMEM((2 * count, width), BF16), pltpu.VMEM((2 * count, width), F32)],
        name="feed_second",
    )(own, pair, weights, weights, before)


def finish_body(scale_by_ref, keep_ref, recv_ref, first_ref, gate_ref, shift_ref, scale_ref, out_w_ref, out_ref):
    share = first_ref.shape[1]
    noise = []
    for i in range(2):
        part = slice(i * share, (i + 1) * share)
        mlp = keep_ref[part] + recv_ref[part].astype(F32)
        total = first_ref[i] + gate_ref[i] * mlp
        fin = (layer_norm(total) * (1.0 + scale_ref[i]) + shift_ref[i]).astype(BF16)
        noise.append(dot(fin, out_w_ref[...]))
    guided = noise[1] + scale_by_ref[0] * (noise[0] - noise[1])
    outs = guided.shape[1]
    wide = jnp.concatenate([guided] * (128 // outs), axis=1)
    wide = jnp.concatenate([wide] * (share * outs // 128), axis=1)
    token = lax.broadcasted_iota(jnp.int32, wide.shape, 0)
    mine = lax.broadcasted_iota(jnp.int32, wide.shape, 1) // outs == token
    out_ref[...] = jnp.sum(jnp.where(mine, wide, 0.0), axis=0, keepdims=True)


def finish(guidance, keep, recv, first_sum, gate_m, shift_f, scale_f, out_local):
    _, share, width = first_sum.shape
    vector = whole((2, 1, width))
    return pl.pallas_call(
        finish_body,
        grid_spec=pltpu.PrefetchScalarGridSpec(
            num_scalar_prefetch=1,
            grid=(1,),
            in_specs=[
                whole(keep.shape),
                whole(recv.shape),
                whole(first_sum.shape),
                vector,
                vector,
                vector,
                whole(out_local.shape),
            ],
            out_specs=whole((1, share * out_local.shape[1])),
        ),
        out_shape=jax.ShapeDtypeStruct((1, share * out_local.shape[1]), F32),
        name="finish",
    )(guidance, keep, recv, first_sum, gate_m, shift_f, scale_f, out_local)


def on_device(
    x_arrive,
    cond_first,
    labels,
    step_ids,
    guidance,
    time_table,
    class_table,
    ada_weight,
    final_ada,
    qkv_weight,
    proj_weight,
    fc1_weight,
    fc2_weight,
    out_weight,
):
    tokens = x_arrive.shape[1]
    width = x_arrive.shape[2]
    rows = qkv_weight.shape[1]
    quarter = qkv_weight.shape[2]
    core = lax.axis_index("group")
    column = lax.axis_index("dp_1")
    high = lax.axis_index("dp_2")
    place = lax.axis_index("mp")
    n_y, n_x, n_z = (lax.axis_size(axis) for axis in DP)
    n_mp = lax.axis_size("mp")
    half = quarter // 2

    time_part = jnp.take(time_table, step_ids, axis=0).astype(F32)
    class_part = jnp.take(class_table, labels, axis=0).astype(F32)
    null_part = class_table[CLASSES].astype(F32)[None, :]
    acts = jax.nn.silu(jnp.concatenate([time_part + class_part, time_part + null_part])).astype(BF16)
    every_act = to_everyone(acts, DP).reshape(-1, acts.shape[1])

    qkv_own = jnp.where(core == 0, qkv_weight[:, :, :half], qkv_weight[:, :, half:])
    qkv_own = qkv_own.transpose(1, 0, 2).reshape(rows, 3 * half)

    shards = jnp.concatenate([fc2_weight.T, fc1_weight, proj_weight.T, qkv_own], axis=1)
    shards = by_height(shards, swap(shards, "dp_2", 1), high)
    qkv_block = shards[:, 2 * width + quarter :]

    def fetch(x, along):
        pairs = [(c * n_mp + m, c * n_mp + (m ^ (2 * c) ^ along)) for c in range(2) for m in range(n_mp)]
        return lax.ppermute(x, ("group", "mp"), pairs)

    feed = fetch(shards[:, : 2 * width + quarter], 0)
    proj_beside = fetch(shards[:, 2 * width : 2 * width + quarter], 1)
    part_a = lanes_full(jnp.concatenate([qkv_block, feed[:, 2 * width :], proj_beside], axis=1))
    part_a, every_act = lax.optimization_barrier((part_a, every_act))
    part_a = gather_y(part_a)
    part_a, every_act = lax.optimization_barrier((part_a, every_act))
    part_a = gather_x(part_a)
    other_a = swap(part_a, "group", 1)

    wide = max(2 * width, -(-GATHER_FLOOR // (2 * n_x * feed.shape[0] * 128)) * 128)
    feed = jnp.pad(feed[:, : 2 * width], ((0, 0), (0, wide - 2 * width)))
    feed = lax.all_gather(feed, "dp_1", axis=0, tiled=True)[:, : 2 * width]
    feed = lax.all_gather(feed, "dp_0", axis=0, tiled=True)
    other_feed = swap(feed, "group", 1)

    mod_part = dot(every_act, ada_weight).astype(BF16)
    mod_part = lax.all_to_all(mod_part, DP, split_axis=0, concat_axis=1, tiled=True)
    final_part = dot(acts, final_ada).astype(BF16)
    mod_parts = to_everyone(jnp.concatenate([mod_part, final_part], axis=1), "mp")

    spot = lax.broadcasted_iota(jnp.int32, (1, width), 1)
    per_x = n_y * n_z * rows
    per_y = n_z * rows
    block = spot // per_x
    inside = spot % per_x
    offset = jnp.where(block == 1, n_x - 1, jnp.where(block == 2, 1, jnp.where(block == 3, 2, 0)))

    from_x = (column + offset) % n_x
    final = (inside // per_y * n_x + from_x) * per_y + inside % per_y
    near_order = (lax.broadcasted_iota(jnp.int32, (width, width), 0) == final).astype(BF16)
    change = (final.reshape(width, 1) == spot).astype(BF16)

    first = cond_first[0] == 1
    cond_rows = jnp.where(first, x_arrive[0], x_arrive[1])
    uncond_rows = jnp.where(first, x_arrive[1], x_arrive[0])
    arrived = jnp.stack([cond_rows, uncond_rows])
    share = tokens // n_mp
    own = lax.dynamic_slice_in_dim(arrived, place * share, share, 1)
    images = dot(arrived.reshape(-1, width), near_order).astype(BF16)
    images = images.reshape(2, tokens, width)
    mod_parts = mod_parts.reshape(n_mp * 2, -1, width)

    turned = dot(mod_parts[:, :2].reshape(-1, width), near_order).reshape(n_mp, 2, 2, 1, width)
    turned = jnp.sum(turned, axis=0)
    shift_a, scale_a = turned[:, 0], turned[:, 1]
    mods = mod_parts[:, 2:].astype(F32).reshape(n_mp, 2, -1, 1, width)
    mods = jnp.sum(mods, axis=0)
    gate_a, shift_m, scale_m, gate_m, shift_f, scale_f = (mods[:, i] for i in range(6))

    cores = core.reshape(1).astype(jnp.int32)
    mixed = attention(cores, images, shift_a, scale_a, part_a, other_a, n_mp, quarter)
    mixed = lax.all_to_all(mixed, "mp", 0, 0, tiled=True)
    base = (place ^ (2 * core)).reshape(1).astype(jnp.int32)
    first_sum, hidden_two = project(base, mixed, part_a, other_a, change, own, gate_a, shift_m, scale_m)
    hidden_two = hidden_two.reshape(2 * share, width)
    pair = swap(hidden_two, "mp", 1)
    before = feed_first(hidden_two, pair, feed)
    keep, send = feed_second(hidden_two, pair, other_feed, before)
    recv = swap(send, "mp", 1)
    return finish(guidance, keep, recv, first_sum, gate_m, shift_f, scale_f, out_weight)


def solution(mesh):
    torus = Mesh(
        mesh.devices.reshape(mesh.shape["group"], 8, 4, 2, mesh.shape["mp"]),
        ("group", "dp_0", "dp_1", "dp_2", "mp"),
    )
    placed = (
        P(GROUP_DP, None, None),
        P(GROUP_DP),
        P(GROUP_DP),
        P(GROUP_DP),
        P(),
        P(None, "mp"),
        P(None, "mp"),
        P("mp", DP),
        P("mp", None),
        P(None, DP, "mp"),
        P("mp", DP),
        P(DP, "mp"),
        P("mp", DP),
        P(),
    )
    return jax.shard_map(on_device, mesh=torus, in_specs=placed, out_specs=P(GROUP_DP, "mp"), check_vma=False)
```

```python
import jax
import jax.numpy as jnp
from jax import lax
from jax.experimental import pallas as pl
from jax.experimental.pallas import tpu as pltpu
from jax.sharding import Mesh
from jax.sharding import PartitionSpec as P

CLASSES = 1000
GATHER_FLOOR = 1 << 20
DP = ("dp_0", "dp_1", "dp_2")
GROUP_DP = ("group", "dp_0", "dp_1", "dp_2")
BF16 = jnp.bfloat16
F32 = jnp.float32


def to_everyone(x, axis):
    size = lax.axis_size(axis)
    return lax.all_to_all(jnp.broadcast_to(x[None], (size, *x.shape)), axis, 0, 0, tiled=True)


def shift(x, axis, step):
    size = lax.axis_size(axis)
    return lax.ppermute(x, axis, [(i, (i + step) % size) for i in range(size)])


def swap(x, axis, bit):
    size = lax.axis_size(axis)
    return lax.ppermute(x, axis, [(i, i ^ bit) for i in range(size)])


def gather_y(block):
    pieces = to_everyone(block, "dp_0")
    return pieces.reshape(pieces.shape[0] * pieces.shape[1], pieces.shape[2])


def gather_x(block):
    half = block.shape[0] // 2
    left = shift(block, "dp_1", 1)
    right = shift(block, "dp_1", -1)
    far_top = shift(left[:half], "dp_1", 1)
    far_bottom = shift(right[half:], "dp_1", -1)
    return jnp.concatenate([block, left, right, far_top, far_bottom], axis=0)


def by_height(own, other, high):
    own_low = high == 0
    return jnp.concatenate([jnp.where(own_low, own, other), jnp.where(own_low, other, own)])


def lanes_full(x):
    return jnp.pad(x, ((0, 0), (0, -x.shape[1] % 128)))


def layer_norm(values):
    mean = jnp.mean(values, axis=-1, keepdims=True)
    centred = values - mean
    spread = jnp.mean(centred * centred, axis=-1, keepdims=True)
    return centred * lax.rsqrt(spread + 1e-06)


def dot(a, b):
    return jnp.dot(a, b, preferred_element_type=F32)


def dot_t(a, b):
    return lax.dot_general(a, b, (((1,), (1,)), ((), ())), preferred_element_type=F32)


def whole(shape):
    return pl.BlockSpec(shape, lambda *_: (0,) * len(shape))


def attention_body(core_ref, x_ref, shift_ref, scale_ref, mine_ref, other_ref, out_ref):
    images, tokens, _ = x_ref.shape
    pieces, quarter, _ = out_ref.shape
    head_dim = quarter // 4
    share = tokens // pieces
    scale = head_dim ** (-0.5)
    low = core_ref[0] == 0
    for image in range(images):
        x = x_ref[image].astype(F32)
        hidden = (layer_norm(x) * (1.0 + scale_ref[image]) + shift_ref[image]).astype(BF16)
        sides = []
        for ref in (mine_ref, other_ref):
            qkv = dot(hidden, ref[:, : 6 * head_dim]).astype(BF16)
            heads = []
            for head in range(2):
                at = head * head_dim
                query = qkv[:, at : at + head_dim]
                keys = qkv[:, 2 * head_dim + at : 3 * head_dim + at]
                values = qkv[:, 4 * head_dim + at : 5 * head_dim + at]
                scores = dot_t(query, keys) * scale
                top = jnp.max(scores, axis=-1, keepdims=True)
                weights = jnp.exp(scores - top)
                total = jnp.sum(weights, axis=-1, keepdims=True)
                probs = (weights * (1.0 / total)).astype(BF16)
                mixed = lax.dot_general(
                    values, probs, (((0,), (1,)), ((), ())), preferred_element_type=F32
                )
                heads.append(mixed.astype(BF16))
            sides.append(jnp.concatenate(heads, axis=0))
        first = jnp.where(low, sides[0], sides[1])
        second = jnp.where(low, sides[1], sides[0])
        mixed = jnp.concatenate([first, second], axis=0)
        for piece in range(pieces):
            part = mixed[:, piece * share : (piece + 1) * share]
            out_ref[piece, :, image * share : (image + 1) * share] = part


def attention(core, x, shift_a, scale_a, mine, other, n_mp, quarter):
    images, tokens, width = x.shape
    vector = whole((images, 1, width))
    out_shape = (n_mp, quarter, images * tokens // n_mp)
    return pl.pallas_call(
        attention_body,
        grid_spec=pltpu.PrefetchScalarGridSpec(
            num_scalar_prefetch=1,
            grid=(1,),
            in_specs=[whole(x.shape), vector, vector, whole(mine.shape), whole(other.shape)],
            out_specs=whole(out_shape),
        ),
        out_shape=jax.ShapeDtypeStruct(out_shape, BF16),
        name="attention",
    )(core, x, shift_a, scale_a, mine, other)


def project_body(base_ref, mixed_ref, mine_ref, other_ref, change_ref, own_ref, gate_ref, shift_ref, scale_ref,
                 sum_ref, hidden_ref, rows_ref):
    quarter = mixed_ref.shape[1]
    start = 3 * quarter // 2
    lead = start % 128
    base = base_ref[0]
    rows_ref[...] = jnp.zeros(rows_ref.shape, BF16)
    for i in range(4):
        at = lead + i % 2 * quarter
        rows_ref[i // 2, at : at + quarter] = mixed_ref[base ^ i]
    attn = dot(mine_ref[:, start - lead :], rows_ref[0])
    attn = (attn + dot(other_ref[:, start - lead :], rows_ref[1])).astype(BF16)
    attn = lax.dot_general(
        attn, change_ref[...], (((0,), (0,)), ((), ())), preferred_element_type=F32
    )
    share = own_ref.shape[1]
    for i in range(2):
        total = own_ref[i].astype(F32) + gate_ref[i] * attn[i * share : (i + 1) * share]
        sum_ref[i] = total
        hidden_ref[i] = (layer_norm(total) * (1.0 + scale_ref[i]) + shift_ref[i]).astype(BF16)


def project(base, mixed, mine, other, change, own, gate_a, shift_m, scale_m):
    _, share, width = own.shape
    vector = whole((2, 1, width))
    start = 3 * mixed.shape[1] // 2
    depth = mine.shape[1] - start // 128 * 128
    return pl.pallas_call(
        project_body,
        grid_spec=pltpu.PrefetchScalarGridSpec(
            num_scalar_prefetch=1,
            grid=(1,),
            in_specs=[
                whole(mixed.shape),
                whole(mine.shape),
                whole(other.shape),
                whole(change.shape),
                whole(own.shape),
                vector,
                vector,
                vector,
            ],
            out_specs=[whole(own.shape), whole(own.shape)],
            scratch_shapes=[pltpu.VMEM((2, depth, 2 * share), BF16)],
        ),
        out_shape=[
            jax.ShapeDtypeStruct(own.shape, F32),
            jax.ShapeDtypeStruct(own.shape, BF16),
        ],
        name="project",
    )(base, mixed, mine, other, change, own, gate_a, shift_m, scale_m)


def feed_part(rows_ref, own_ref, pair_ref, up_ref, down_ref, so_far):
    count = own_ref.shape[0]

    @pl.when(pl.program_id(0) == 0)
    def _():
        rows_ref[:count] = own_ref[...]
        rows_ref[count:] = pair_ref[...]

    hidden = jax.nn.gelu(dot(rows_ref[...], up_ref[...]), approximate=True).astype(BF16)
    return so_far() + dot_t(down_ref[...], hidden)


def feed_first_body(own_ref, pair_ref, up_ref, down_ref, sum_ref, rows_ref):
    @pl.when(pl.program_id(0) == 0)
    def _():
        sum_ref[...] = jnp.zeros(sum_ref.shape, F32)

    sum_ref[...] = feed_part(rows_ref, own_ref, pair_ref, up_ref, down_ref, lambda: sum_ref[...])


def feed_second_body(own_ref, pair_ref, up_ref, down_ref, before_ref, keep_ref, send_ref, rows_ref, sum_ref):
    count = own_ref.shape[0]

    @pl.when(pl.program_id(0) == 0)
    def _():
        sum_ref[...] = before_ref[...]

    sum_ref[...] = feed_part(rows_ref, own_ref, pair_ref, up_ref, down_ref, lambda: sum_ref[...])

    @pl.when(pl.program_id(0) == pl.num_programs(0) - 1)
    def _():
        total = sum_ref[...].T
        keep_ref[...] = total[:count]
        send_ref[...] = total[count:].astype(BF16)


def feed_first(own, pair, weights):
    count, width = own.shape
    steps = 3
    up = pl.BlockSpec((width, width // steps), lambda i: (0, steps + i))
    down = pl.BlockSpec((width, width // steps), lambda i: (0, i))
    return pl.pallas_call(
        feed_first_body,
        grid=(steps,),
        in_specs=[whole(own.shape), whole(own.shape), up, down],
        out_specs=whole((width, 2 * count)),
        out_shape=jax.ShapeDtypeStruct((width, 2 * count), F32),
        scratch_shapes=[pltpu.VMEM((2 * count, width), BF16)],
        name="feed_first",
    )(own, pair, weights, weights)


def feed_second(own, pair, weights, before):
    count, width = own.shape
    steps = 3
    up = pl.BlockSpec((width, width // steps), lambda i: (0, steps + i))
    down = pl.BlockSpec((width, width // steps), lambda i: (0, i))
    return pl.pallas_call(
        feed_second_body,
        grid=(steps,),
        in_specs=[whole(own.shape), whole(own.shape), up, down, whole(before.shape)],
        out_specs=[whole(own.shape), whole(own.shape)],
        out_shape=[
            jax.ShapeDtypeStruct(own.shape, F32),
            jax.ShapeDtypeStruct(own.shape, BF16),
        ],
        scratch_shapes=[pltpu.VMEM((2 * count, width), BF16), pltpu.VMEM((width, 2 * count), F32)],
        name="feed_second",
    )(own, pair, weights, weights, before)


def finish_body(scale_by_ref, keep_ref, recv_ref, first_ref, gate_ref, shift_ref, scale_ref, out_w_ref, out_ref):
    share = first_ref.shape[1]
    noise = []
    for i in range(2):
        part = slice(i * share, (i + 1) * share)
        mlp = keep_ref[part] + recv_ref[part].astype(F32)
        total = first_ref[i] + gate_ref[i] * mlp
        fin = (layer_norm(total) * (1.0 + scale_ref[i]) + shift_ref[i]).astype(BF16)
        noise.append(dot(fin, out_w_ref[...]))
    guided = noise[1] + scale_by_ref[0] * (noise[0] - noise[1])
    outs = guided.shape[1]
    wide = jnp.concatenate([guided] * (128 // outs), axis=1)
    wide = jnp.concatenate([wide] * (share * outs // 128), axis=1)
    token = lax.broadcasted_iota(jnp.int32, wide.shape, 0)
    mine = lax.broadcasted_iota(jnp.int32, wide.shape, 1) // outs == token
    out_ref[...] = jnp.sum(jnp.where(mine, wide, 0.0), axis=0, keepdims=True)


def finish(guidance, keep, recv, first_sum, gate_m, shift_f, scale_f, out_local):
    _, share, width = first_sum.shape
    vector = whole((2, 1, width))
    return pl.pallas_call(
        finish_body,
        grid_spec=pltpu.PrefetchScalarGridSpec(
            num_scalar_prefetch=1,
            grid=(1,),
            in_specs=[
                whole(keep.shape),
                whole(recv.shape),
                whole(first_sum.shape),
                vector,
                vector,
                vector,
                whole(out_local.shape),
            ],
            out_specs=whole((1, share * out_local.shape[1])),
        ),
        out_shape=jax.ShapeDtypeStruct((1, share * out_local.shape[1]), F32),
        name="finish",
    )(guidance, keep, recv, first_sum, gate_m, shift_f, scale_f, out_local)


def on_device(
    x_arrive,
    cond_first,
    labels,
    step_ids,
    guidance,
    time_table,
    class_table,
    ada_weight,
    final_ada,
    qkv_weight,
    proj_weight,
    fc1_weight,
    fc2_weight,
    out_weight,
):
    tokens = x_arrive.shape[1]
    width = x_arrive.shape[2]
    rows = qkv_weight.shape[1]
    quarter = qkv_weight.shape[2]
    core = lax.axis_index("group")
    column = lax.axis_index("dp_1")
    high = lax.axis_index("dp_2")
    place = lax.axis_index("mp")
    n_y, n_x, n_z = (lax.axis_size(axis) for axis in DP)
    n_mp = lax.axis_size("mp")
    half = quarter // 2

    time_part = jnp.take(time_table, step_ids, axis=0).astype(F32)
    class_part = jnp.take(class_table, labels, axis=0).astype(F32)
    null_part = class_table[CLASSES].astype(F32)[None, :]
    acts = jax.nn.silu(jnp.concatenate([time_part + class_part, time_part + null_part])).astype(BF16)
    every_act = to_everyone(acts, DP).reshape(-1, acts.shape[1])

    qkv_own = jnp.where(core == 0, qkv_weight[:, :, :half], qkv_weight[:, :, half:])
    qkv_own = qkv_own.transpose(1, 0, 2).reshape(rows, 3 * half)

    shards = jnp.concatenate([fc2_weight.T, fc1_weight, proj_weight.T, qkv_own], axis=1)
    shards = by_height(shards, swap(shards, "dp_2", 1), high)
    qkv_block = shards[:, 2 * width + quarter :]

    def fetch(x, along):
        pairs = [(c * n_mp + m, c * n_mp + (m ^ (2 * c) ^ along)) for c in range(2) for m in range(n_mp)]
        return lax.ppermute(x, ("group", "mp"), pairs)

    feed = fetch(shards[:, : 2 * width + quarter], 0)
    proj_beside = fetch(shards[:, 2 * width : 2 * width + quarter], 1)
    part_a = lanes_full(jnp.concatenate([qkv_block, feed[:, 2 * width :], proj_beside], axis=1))
    part_a, every_act = lax.optimization_barrier((part_a, every_act))
    part_a = gather_y(part_a)
    part_a, every_act = lax.optimization_barrier((part_a, every_act))
    part_a = gather_x(part_a)
    other_a = swap(part_a, "group", 1)

    wide = max(2 * width, -(-GATHER_FLOOR // (2 * n_x * feed.shape[0] * 128)) * 128)
    feed = jnp.pad(feed[:, : 2 * width], ((0, 0), (0, wide - 2 * width)))
    feed = lax.all_gather(feed, "dp_1", axis=0, tiled=True)[:, : 2 * width]
    feed = lax.all_gather(feed, "dp_0", axis=0, tiled=True)
    other_feed = swap(feed, "group", 1)

    mod_part = dot(every_act, ada_weight).astype(BF16)
    mod_part = lax.all_to_all(mod_part, DP, split_axis=0, concat_axis=1, tiled=True)
    final_part = dot(acts, final_ada).astype(BF16)
    mod_parts = to_everyone(jnp.concatenate([mod_part, final_part], axis=1), "mp")

    spot = lax.broadcasted_iota(jnp.int32, (1, width), 1)
    per_x = n_y * n_z * rows
    per_y = n_z * rows
    block = spot // per_x
    inside = spot % per_x
    offset = jnp.where(block == 1, n_x - 1, jnp.where(block == 2, 1, jnp.where(block == 3, 2, 0)))

    from_x = (column + offset) % n_x
    final = (inside // per_y * n_x + from_x) * per_y + inside % per_y
    near_order = (lax.broadcasted_iota(jnp.int32, (width, width), 0) == final).astype(BF16)
    change = (final.reshape(width, 1) == spot).astype(BF16)

    first = cond_first[0] == 1
    cond_rows = jnp.where(first, x_arrive[0], x_arrive[1])
    uncond_rows = jnp.where(first, x_arrive[1], x_arrive[0])
    arrived = jnp.stack([cond_rows, uncond_rows])
    share = tokens // n_mp
    own = lax.dynamic_slice_in_dim(arrived, place * share, share, 1)
    images = dot(arrived.reshape(-1, width), near_order).astype(BF16)
    images = images.reshape(2, tokens, width)
    mod_parts = mod_parts.reshape(n_mp * 2, -1, width)

    turned = dot(mod_parts[:, :2].reshape(-1, width), near_order).reshape(n_mp, 2, 2, 1, width)
    turned = jnp.sum(turned, axis=0)
    shift_a, scale_a = turned[:, 0], turned[:, 1]
    mods = mod_parts[:, 2:].astype(F32).reshape(n_mp, 2, -1, 1, width)
    mods = jnp.sum(mods, axis=0)
    gate_a, shift_m, scale_m, gate_m, shift_f, scale_f = (mods[:, i] for i in range(6))

    cores = core.reshape(1).astype(jnp.int32)
    mixed = attention(cores, images, shift_a, scale_a, part_a, other_a, n_mp, quarter)
    mixed = lax.all_to_all(mixed, "mp", 0, 0, tiled=True)
    base = (place ^ (2 * core)).reshape(1).astype(jnp.int32)
    first_sum, hidden_two = project(base, mixed, part_a, other_a, change, own, gate_a, shift_m, scale_m)
    hidden_two = hidden_two.reshape(2 * share, width)
    pair = swap(hidden_two, "mp", 1)
    before = feed_first(hidden_two, pair, feed)
    keep, send = feed_second(hidden_two, pair, other_feed, before)
    recv = swap(send, "mp", 1)
    return finish(guidance, keep, recv, first_sum, gate_m, shift_f, scale_f, out_weight)


def solution(mesh):
    torus = Mesh(
        mesh.devices.reshape(mesh.shape["group"], 8, 4, 2, mesh.shape["mp"]),
        ("group", "dp_0", "dp_1", "dp_2", "mp"),
    )
    placed = (
        P(GROUP_DP, None, None),
        P(GROUP_DP),
        P(GROUP_DP),
        P(GROUP_DP),
        P(),
        P(None, "mp"),
        P(None, "mp"),
        P("mp", DP),
        P("mp", None),
        P(None, DP, "mp"),
        P("mp", DP),
        P(DP, "mp"),
        P("mp", DP),
        P(),
    )
    return jax.shard_map(on_device, mesh=torus, in_specs=placed, out_specs=P(GROUP_DP, "mp"), check_vma=False)
```

```python
import jax
import jax.numpy as jnp
from jax import lax
from jax.experimental import pallas as pl
from jax.experimental.pallas import tpu as pltpu
from jax.sharding import Mesh
from jax.sharding import PartitionSpec as P

CLASSES = 1000
GATHER_FLOOR = 1 << 20
DP = ("dp_0", "dp_1", "dp_2")
GROUP_DP = ("group", "dp_0", "dp_1", "dp_2")
BF16 = jnp.bfloat16
F32 = jnp.float32


def to_everyone(x, axis):
    size = lax.axis_size(axis)
    return lax.all_to_all(jnp.broadcast_to(x[None], (size, *x.shape)), axis, 0, 0, tiled=True)


def shift(x, axis, step):
    size = lax.axis_size(axis)
    return lax.ppermute(x, axis, [(i, (i + step) % size) for i in range(size)])


def swap(x, axis, bit):
    size = lax.axis_size(axis)
    return lax.ppermute(x, axis, [(i, i ^ bit) for i in range(size)])


def gather_y(block):
    pieces = to_everyone(block, "dp_0")
    return pieces.reshape(pieces.shape[0] * pieces.shape[1], pieces.shape[2])


def gather_x(block):
    half = block.shape[0] // 2
    left = shift(block, "dp_1", 1)
    right = shift(block, "dp_1", -1)
    far_top = shift(left[:half], "dp_1", 1)
    far_bottom = shift(right[half:], "dp_1", -1)
    return jnp.concatenate([block, left, right, far_top, far_bottom], axis=0)


def by_height(own, other, high):
    own_low = high == 0
    return jnp.concatenate([jnp.where(own_low, own, other), jnp.where(own_low, other, own)])


def lanes_full(x):
    return jnp.pad(x, ((0, 0), (0, -x.shape[1] % 128)))


def layer_norm(values):
    mean = jnp.mean(values, axis=-1, keepdims=True)
    centred = values - mean
    spread = jnp.mean(centred * centred, axis=-1, keepdims=True)
    return centred * lax.rsqrt(spread + 1e-06)


def dot(a, b):
    return jnp.dot(a, b, preferred_element_type=F32)


def dot_t(a, b):
    return lax.dot_general(a, b, (((1,), (1,)), ((), ())), preferred_element_type=F32)


def whole(shape):
    return pl.BlockSpec(shape, lambda *_: (0,) * len(shape))


def attention_body(core_ref, x_ref, shift_ref, scale_ref, mine_ref, other_ref, out_ref):
    images, tokens, _ = x_ref.shape
    pieces, quarter, _ = out_ref.shape
    head_dim = quarter // 4
    share = tokens // pieces
    scale = head_dim ** (-0.5)
    low = core_ref[0] == 0
    for image in range(images):
        x = x_ref[image].astype(F32)
        hidden = (layer_norm(x) * (1.0 + scale_ref[image]) + shift_ref[image]).astype(BF16)
        sides = []
        for ref in (mine_ref, other_ref):
            qkv = dot(hidden, ref[:, : 6 * head_dim]).astype(BF16)
            heads = []
            for head in range(2):
                at = head * head_dim
                query = qkv[:, at : at + head_dim]
                keys = qkv[:, 2 * head_dim + at : 3 * head_dim + at]
                values = qkv[:, 4 * head_dim + at : 5 * head_dim + at]
                scores = dot_t(query, keys) * scale
                top = jnp.max(scores, axis=-1, keepdims=True)
                weights = jnp.exp(scores - top)
                total = jnp.sum(weights, axis=-1, keepdims=True)
                probs = (weights * (1.0 / total)).astype(BF16)
                mixed = lax.dot_general(
                    values, probs, (((0,), (1,)), ((), ())), preferred_element_type=F32
                )
                heads.append(mixed.astype(BF16))
            sides.append(jnp.concatenate(heads, axis=0))
        first = jnp.where(low, sides[0], sides[1])
        second = jnp.where(low, sides[1], sides[0])
        mixed = jnp.concatenate([first, second], axis=0)
        for piece in range(pieces):
            part = mixed[:, piece * share : (piece + 1) * share]
            out_ref[piece, :, image * share : (image + 1) * share] = part


def attention(core, x, shift_a, scale_a, mine, other, n_mp, quarter):
    images, tokens, width = x.shape
    vector = whole((images, 1, width))
    out_shape = (n_mp, quarter, images * tokens // n_mp)
    lanes = whole((width, -(-3 * quarter // 2 // 128) * 128))
    return pl.pallas_call(
        attention_body,
        grid_spec=pltpu.PrefetchScalarGridSpec(
            num_scalar_prefetch=1,
            grid=(1,),
            in_specs=[whole(x.shape), vector, vector, lanes, lanes],
            out_specs=whole(out_shape),
        ),
        out_shape=jax.ShapeDtypeStruct(out_shape, BF16),
        name="attention",
        compiler_params=pltpu.CompilerParams(vmem_limit_bytes=20 << 20),
    )(core, x, shift_a, scale_a, mine, other)


def project_body(base_ref, mixed_ref, mine_ref, other_ref, change_ref, own_ref, gate_ref, shift_ref, scale_ref,
                 sum_ref, hidden_ref, rows_ref):
    quarter = mixed_ref.shape[1]
    start = 3 * quarter // 2
    lead = start % 128
    base = base_ref[0]
    rows_ref[...] = jnp.zeros(rows_ref.shape, BF16)
    for i in range(4):
        at = lead + i % 2 * quarter
        rows_ref[i // 2, at : at + quarter] = mixed_ref[base ^ i]
    attn = dot(mine_ref[...], rows_ref[0])
    attn = (attn + dot(other_ref[...], rows_ref[1])).astype(BF16)
    attn = lax.dot_general(
        attn, change_ref[...], (((0,), (0,)), ((), ())), preferred_element_type=F32
    )
    share = own_ref.shape[1]
    for i in range(2):
        total = own_ref[i].astype(F32) + gate_ref[i] * attn[i * share : (i + 1) * share]
        sum_ref[i] = total
        hidden_ref[i] = (layer_norm(total) * (1.0 + scale_ref[i]) + shift_ref[i]).astype(BF16)


def project(base, mixed, mine, other, change, own, gate_a, shift_m, scale_m):
    _, share, width = own.shape
    vector = whole((2, 1, width))
    start = 3 * mixed.shape[1] // 2
    depth = mine.shape[1] - start // 128 * 128
    lanes = pl.BlockSpec(
        (pl.Element(width), pl.Element(depth)), lambda *_: (0, start // 128 * 128)
    )
    return pl.pallas_call(
        project_body,
        grid_spec=pltpu.PrefetchScalarGridSpec(
            num_scalar_prefetch=1,
            grid=(1,),
            in_specs=[
                whole(mixed.shape),
                lanes,
                lanes,
                whole(change.shape),
                whole(own.shape),
                vector,
                vector,
                vector,
            ],
            out_specs=[whole(own.shape), whole(own.shape)],
            scratch_shapes=[pltpu.VMEM((2, depth, 2 * share), BF16)],
        ),
        out_shape=[
            jax.ShapeDtypeStruct(own.shape, F32),
            jax.ShapeDtypeStruct(own.shape, BF16),
        ],
        name="project",
        compiler_params=pltpu.CompilerParams(vmem_limit_bytes=20 << 20),
    )(base, mixed, mine, other, change, own, gate_a, shift_m, scale_m)


def feed_part(rows_ref, own_ref, pair_ref, up_ref, down_ref, so_far):
    count = own_ref.shape[0]

    @pl.when(pl.program_id(0) == 0)
    def _():
        rows_ref[:count] = own_ref[...]
        rows_ref[count:] = pair_ref[...]

    hidden = jax.nn.gelu(dot(rows_ref[...], up_ref[...]), approximate=True).astype(BF16)
    return so_far() + dot_t(down_ref[...], hidden)


def feed_first_body(own_ref, pair_ref, up_ref, down_ref, sum_ref, rows_ref):
    @pl.when(pl.program_id(0) == 0)
    def _():
        sum_ref[...] = jnp.zeros(sum_ref.shape, F32)

    sum_ref[...] = feed_part(rows_ref, own_ref, pair_ref, up_ref, down_ref, lambda: sum_ref[...])


def feed_second_body(own_ref, pair_ref, up_ref, down_ref, before_ref, keep_ref, send_ref, rows_ref, sum_ref):
    count = own_ref.shape[0]

    @pl.when(pl.program_id(0) == 0)
    def _():
        sum_ref[...] = before_ref[...]

    sum_ref[...] = feed_part(rows_ref, own_ref, pair_ref, up_ref, down_ref, lambda: sum_ref[...])

    @pl.when(pl.program_id(0) == pl.num_programs(0) - 1)
    def _():
        total = sum_ref[...].T
        keep_ref[...] = total[:count]
        send_ref[...] = total[count:].astype(BF16)


def feed_first(own, pair, weights):
    count, width = own.shape
    steps = 3
    up = pl.BlockSpec((width, width // steps), lambda i: (0, steps + i))
    down = pl.BlockSpec((width, width // steps), lambda i: (0, i))
    return pl.pallas_call(
        feed_first_body,
        grid=(steps,),
        in_specs=[whole(own.shape), whole(own.shape), up, down],
        out_specs=whole((width, 2 * count)),
        out_shape=jax.ShapeDtypeStruct((width, 2 * count), F32),
        scratch_shapes=[pltpu.VMEM((2 * count, width), BF16)],
        name="feed_first",
        compiler_params=pltpu.CompilerParams(vmem_limit_bytes=20 << 20),
    )(own, pair, weights, weights)


def feed_second(own, pair, weights, before):
    count, width = own.shape
    steps = 3
    up = pl.BlockSpec((width, width // steps), lambda i: (0, steps + i))
    down = pl.BlockSpec((width, width // steps), lambda i: (0, i))
    return pl.pallas_call(
        feed_second_body,
        grid=(steps,),
        in_specs=[whole(own.shape), whole(own.shape), up, down, whole(before.shape)],
        out_specs=[whole(own.shape), whole(own.shape)],
        out_shape=[
            jax.ShapeDtypeStruct(own.shape, F32),
            jax.ShapeDtypeStruct(own.shape, BF16),
        ],
        scratch_shapes=[pltpu.VMEM((2 * count, width), BF16), pltpu.VMEM((width, 2 * count), F32)],
        name="feed_second",
        compiler_params=pltpu.CompilerParams(vmem_limit_bytes=20 << 20),
    )(own, pair, weights, weights, before)


def finish_body(scale_by_ref, keep_ref, recv_ref, first_ref, gate_ref, shift_ref, scale_ref, out_w_ref, out_ref):
    share = first_ref.shape[1]
    noise = []
    for i in range(2):
        part = slice(i * share, (i + 1) * share)
        mlp = keep_ref[part] + recv_ref[part].astype(F32)
        total = first_ref[i] + gate_ref[i] * mlp
        fin = (layer_norm(total) * (1.0 + scale_ref[i]) + shift_ref[i]).astype(BF16)
        noise.append(dot(fin, out_w_ref[...]))
    guided = noise[1] + scale_by_ref[0] * (noise[0] - noise[1])
    outs = guided.shape[1]
    wide = jnp.concatenate([guided] * (128 // outs), axis=1)
    wide = jnp.concatenate([wide] * (share * outs // 128), axis=1)
    token = lax.broadcasted_iota(jnp.int32, wide.shape, 0)
    mine = lax.broadcasted_iota(jnp.int32, wide.shape, 1) // outs == token
    out_ref[...] = jnp.sum(jnp.where(mine, wide, 0.0), axis=0, keepdims=True)


def finish(guidance, keep, recv, first_sum, gate_m, shift_f, scale_f, out_local):
    _, share, width = first_sum.shape
    vector = whole((2, 1, width))
    return pl.pallas_call(
        finish_body,
        grid_spec=pltpu.PrefetchScalarGridSpec(
            num_scalar_prefetch=1,
            grid=(1,),
            in_specs=[
                whole(keep.shape),
                whole(recv.shape),
                whole(first_sum.shape),
                vector,
                vector,
                vector,
                whole(out_local.shape),
            ],
            out_specs=whole((1, share * out_local.shape[1])),
        ),
        out_shape=jax.ShapeDtypeStruct((1, share * out_local.shape[1]), F32),
        name="finish",
        compiler_params=pltpu.CompilerParams(vmem_limit_bytes=20 << 20),
    )(guidance, keep, recv, first_sum, gate_m, shift_f, scale_f, out_local)


def on_device(
    x_arrive,
    cond_first,
    labels,
    step_ids,
    guidance,
    time_table,
    class_table,
    ada_weight,
    final_ada,
    qkv_weight,
    proj_weight,
    fc1_weight,
    fc2_weight,
    out_weight,
):
    tokens = x_arrive.shape[1]
    width = x_arrive.shape[2]
    rows = qkv_weight.shape[1]
    quarter = qkv_weight.shape[2]
    core = lax.axis_index("group")
    column = lax.axis_index("dp_1")
    high = lax.axis_index("dp_2")
    place = lax.axis_index("mp")
    n_y, n_x, n_z = (lax.axis_size(axis) for axis in DP)
    n_mp = lax.axis_size("mp")
    half = quarter // 2

    time_part = jnp.take(time_table, step_ids, axis=0).astype(F32)
    class_part = jnp.take(class_table, labels, axis=0).astype(F32)
    null_part = class_table[CLASSES].astype(F32)[None, :]
    acts = jax.nn.silu(jnp.concatenate([time_part + class_part, time_part + null_part])).astype(BF16)
    every_act = to_everyone(acts, DP).reshape(-1, acts.shape[1])

    qkv_own = jnp.where(core == 0, qkv_weight[:, :, :half], qkv_weight[:, :, half:])
    qkv_own = qkv_own.transpose(1, 0, 2).reshape(rows, 3 * half)

    shards = jnp.concatenate([fc2_weight.T, fc1_weight, proj_weight.T, qkv_own], axis=1)
    shards = by_height(shards, swap(shards, "dp_2", 1), high)
    qkv_block = shards[:, 2 * width + quarter :]

    def fetch(x, along):
        pairs = [(c * n_mp + m, c * n_mp + (m ^ (2 * c) ^ along)) for c in range(2) for m in range(n_mp)]
        return lax.ppermute(x, ("group", "mp"), pairs)

    feed = fetch(shards[:, : 2 * width + quarter], 0)
    proj_beside = fetch(shards[:, 2 * width : 2 * width + quarter], 1)
    part_a = lanes_full(jnp.concatenate([qkv_block, feed[:, 2 * width :], proj_beside], axis=1))
    part_a, every_act = lax.optimization_barrier((part_a, every_act))
    part_a = gather_y(part_a)
    part_a, every_act = lax.optimization_barrier((part_a, every_act))
    part_a = gather_x(part_a)
    other_a = swap(part_a, "group", 1)

    wide = max(2 * width, -(-GATHER_FLOOR // (2 * n_x * feed.shape[0] * 128)) * 128)
    feed = jnp.pad(feed[:, : 2 * width], ((0, 0), (0, wide - 2 * width)))
    feed = lax.all_gather(feed, "dp_1", axis=0)
    feed = feed[:, :, : 2 * width].reshape(-1, 2 * width)
    feed = lax.all_gather(feed, "dp_0", axis=0, tiled=True)
    other_feed = swap(feed, "group", 1)

    mod_part = dot(every_act, ada_weight).astype(BF16)
    mod_part = lax.all_to_all(mod_part, DP, split_axis=0, concat_axis=1, tiled=True)
    final_part = dot(acts, final_ada).astype(BF16)
    mod_parts = to_everyone(jnp.concatenate([mod_part, final_part], axis=1), "mp")

    spot = lax.broadcasted_iota(jnp.int32, (1, width), 1)
    per_x = n_y * n_z * rows
    per_y = n_z * rows
    block = spot // per_x
    inside = spot % per_x
    offset = jnp.where(block == 1, n_x - 1, jnp.where(block == 2, 1, jnp.where(block == 3, 2, 0)))

    from_x = (column + offset) % n_x
    final = (inside // per_y * n_x + from_x) * per_y + inside % per_y
    near_order = (lax.broadcasted_iota(jnp.int32, (width, width), 0) == final).astype(BF16)
    change = (final.reshape(width, 1) == spot).astype(BF16)

    first = cond_first[0] == 1
    cond_rows = jnp.where(first, x_arrive[0], x_arrive[1])
    uncond_rows = jnp.where(first, x_arrive[1], x_arrive[0])
    arrived = jnp.stack([cond_rows, uncond_rows])
    share = tokens // n_mp
    own = lax.dynamic_slice_in_dim(arrived, place * share, share, 1)
    images = dot(arrived.reshape(-1, width), near_order).astype(BF16)
    images = images.reshape(2, tokens, width)
    mod_parts = mod_parts.reshape(n_mp * 2, -1, width)

    turned = dot(mod_parts[:, :2].reshape(-1, width), near_order).reshape(n_mp, 2, 2, 1, width)
    turned = jnp.sum(turned, axis=0)
    shift_a, scale_a = turned[:, 0], turned[:, 1]
    mods = mod_parts[:, 2:].astype(F32).reshape(n_mp, 2, -1, 1, width)
    mods = jnp.sum(mods, axis=0)
    gate_a, shift_m, scale_m, gate_m, shift_f, scale_f = (mods[:, i] for i in range(6))

    cores = core.reshape(1).astype(jnp.int32)
    mixed = attention(cores, images, shift_a, scale_a, part_a, other_a, n_mp, quarter)
    mixed = lax.all_to_all(mixed, "mp", 0, 0, tiled=True)
    base = (place ^ (2 * core)).reshape(1).astype(jnp.int32)
    first_sum, hidden_two = project(base, mixed, part_a, other_a, change, own, gate_a, shift_m, scale_m)
    hidden_two = hidden_two.reshape(2 * share, width)
    pair = swap(hidden_two, "mp", 1)
    before = feed_first(hidden_two, pair, feed)
    keep, send = feed_second(hidden_two, pair, other_feed, before)
    recv = swap(send, "mp", 1)
    return finish(guidance, keep, recv, first_sum, gate_m, shift_f, scale_f, out_weight)


def solution(mesh):
    torus = Mesh(
        mesh.devices.reshape(mesh.shape["group"], 8, 4, 2, mesh.shape["mp"]),
        ("group", "dp_0", "dp_1", "dp_2", "mp"),
    )
    placed = (
        P(GROUP_DP, None, None),
        P(GROUP_DP),
        P(GROUP_DP),
        P(GROUP_DP),
        P(),
        P(None, "mp"),
        P(None, "mp"),
        P("mp", DP),
        P("mp", None),
        P(None, DP, "mp"),
        P("mp", DP),
        P(DP, "mp"),
        P("mp", DP),
        P(),
    )
    return jax.shard_map(on_device, mesh=torus, in_specs=placed, out_specs=P(GROUP_DP, "mp"), check_vma=False)
```

```python
import jax
import jax.numpy as jnp
from jax import lax
from jax.experimental import pallas as pl
from jax.experimental.pallas import tpu as pltpu
from jax.sharding import Mesh
from jax.sharding import PartitionSpec as P

CLASSES = 1000
GATHER_FLOOR = 1 << 20
DP = ("dp_0", "dp_1", "dp_2")
GROUP_DP = ("group", "dp_0", "dp_1", "dp_2")
BF16 = jnp.bfloat16
F32 = jnp.float32


def to_everyone(x, axis):
    size = lax.axis_size(axis)
    return lax.all_to_all(jnp.broadcast_to(x[None], (size, *x.shape)), axis, 0, 0, tiled=True)


def shift(x, axis, step):
    size = lax.axis_size(axis)
    return lax.ppermute(x, axis, [(i, (i + step) % size) for i in range(size)])


def swap(x, axis, bit):
    size = lax.axis_size(axis)
    return lax.ppermute(x, axis, [(i, i ^ bit) for i in range(size)])


def gather_y(block):
    pieces = to_everyone(block, "dp_0")
    return pieces.reshape(pieces.shape[0] * pieces.shape[1], pieces.shape[2])


def gather_x(block):
    half = block.shape[0] // 2
    left = shift(block, "dp_1", 1)
    right = shift(block, "dp_1", -1)
    far_top = shift(left[:half], "dp_1", 1)
    far_bottom = shift(right[half:], "dp_1", -1)
    return jnp.concatenate([block, left, right, far_top, far_bottom], axis=0)


def by_height(own, other, high):
    own_low = high == 0
    return jnp.concatenate([jnp.where(own_low, own, other), jnp.where(own_low, other, own)])


def lanes_full(x):
    return jnp.pad(x, ((0, 0), (0, -x.shape[1] % 128)))


def layer_norm(values):
    mean = jnp.mean(values, axis=-1, keepdims=True)
    centred = values - mean
    spread = jnp.mean(centred * centred, axis=-1, keepdims=True)
    return centred * lax.rsqrt(spread + 1e-06)


def dot(a, b):
    return jnp.dot(a, b, preferred_element_type=F32)


def dot_t(a, b):
    return lax.dot_general(a, b, (((1,), (1,)), ((), ())), preferred_element_type=F32)


def whole(shape):
    return pl.BlockSpec(shape, lambda *_: (0,) * len(shape))


def attention_body(core_ref, x_ref, shift_ref, scale_ref, mine_ref, other_ref, out_ref):
    images, tokens, _ = x_ref.shape
    pieces, quarter, _ = out_ref.shape
    head_dim = quarter // 4
    share = tokens // pieces
    scale = head_dim ** (-0.5)
    low = core_ref[0] == 0
    for image in range(images):
        x = x_ref[image].astype(F32)
        hidden = (layer_norm(x) * (1.0 + scale_ref[image]) + shift_ref[image]).astype(BF16)
        sides = []
        for ref in (mine_ref, other_ref):
            qkv = dot(hidden, ref[:, : 6 * head_dim]).astype(BF16)
            heads = []
            for head in range(2):
                at = head * head_dim
                query = qkv[:, at : at + head_dim]
                keys = qkv[:, 2 * head_dim + at : 3 * head_dim + at]
                values = qkv[:, 4 * head_dim + at : 5 * head_dim + at]
                scores = dot_t(query, keys) * scale
                top = jnp.max(scores, axis=-1, keepdims=True)
                weights = jnp.exp(scores - top)
                total = jnp.sum(weights, axis=-1, keepdims=True)
                probs = (weights * (1.0 / total)).astype(BF16)
                mixed = lax.dot_general(
                    values, probs, (((0,), (1,)), ((), ())), preferred_element_type=F32
                )
                heads.append(mixed.astype(BF16))
            sides.append(jnp.concatenate(heads, axis=0))
        first = jnp.where(low, sides[0], sides[1])
        second = jnp.where(low, sides[1], sides[0])
        mixed = jnp.concatenate([first, second], axis=0)
        for piece in range(pieces):
            part = mixed[:, piece * share : (piece + 1) * share]
            out_ref[piece, :, image * share : (image + 1) * share] = part


def attention(core, x, shift_a, scale_a, mine, other, n_mp, quarter):
    images, tokens, width = x.shape
    vector = whole((images, 1, width))
    out_shape = (n_mp, quarter, images * tokens // n_mp)
    lanes = whole((width, -(-3 * quarter // 2 // 128) * 128))
    return pl.pallas_call(
        attention_body,
        grid_spec=pltpu.PrefetchScalarGridSpec(
            num_scalar_prefetch=1,
            grid=(1,),
            in_specs=[whole(x.shape), vector, vector, lanes, lanes],
            out_specs=whole(out_shape),
        ),
        out_shape=jax.ShapeDtypeStruct(out_shape, BF16),
        name="attention",
        compiler_params=pltpu.CompilerParams(vmem_limit_bytes=20 << 20),
    )(core, x, shift_a, scale_a, mine, other)


def project_body(base_ref, mixed_ref, mine_ref, other_ref, change_ref, own_ref, gate_ref, shift_ref, scale_ref,
                 sum_ref, hidden_ref, rows_ref):
    quarter = mixed_ref.shape[1]
    start = 3 * quarter // 2
    lead = start % 128
    base = base_ref[0]
    rows_ref[...] = jnp.zeros(rows_ref.shape, BF16)
    for i in range(4):
        at = lead + i % 2 * quarter
        rows_ref[i // 2, at : at + quarter] = mixed_ref[base ^ i]
    attn = dot(mine_ref[...], rows_ref[0])
    attn = (attn + dot(other_ref[...], rows_ref[1])).astype(BF16)
    attn = lax.dot_general(
        attn, change_ref[...], (((0,), (0,)), ((), ())), preferred_element_type=F32
    )
    share = own_ref.shape[1]
    for i in range(2):
        total = own_ref[i].astype(F32) + gate_ref[i] * attn[i * share : (i + 1) * share]
        sum_ref[i] = total
        hidden_ref[i] = (layer_norm(total) * (1.0 + scale_ref[i]) + shift_ref[i]).astype(BF16)


def project(base, mixed, mine, other, change, own, gate_a, shift_m, scale_m):
    _, share, width = own.shape
    vector = whole((2, 1, width))
    start = 3 * mixed.shape[1] // 2
    depth = mine.shape[1] - start // 128 * 128
    lanes = pl.BlockSpec(
        (pl.Element(width), pl.Element(depth)), lambda *_: (0, start // 128 * 128)
    )
    return pl.pallas_call(
        project_body,
        grid_spec=pltpu.PrefetchScalarGridSpec(
            num_scalar_prefetch=1,
            grid=(1,),
            in_specs=[
                whole(mixed.shape),
                lanes,
                lanes,
                whole(change.shape),
                whole(own.shape),
                vector,
                vector,
                vector,
            ],
            out_specs=[whole(own.shape), whole(own.shape)],
            scratch_shapes=[pltpu.VMEM((2, depth, 2 * share), BF16)],
        ),
        out_shape=[
            jax.ShapeDtypeStruct(own.shape, F32),
            jax.ShapeDtypeStruct(own.shape, BF16),
        ],
        name="project",
        compiler_params=pltpu.CompilerParams(vmem_limit_bytes=20 << 20),
    )(base, mixed, mine, other, change, own, gate_a, shift_m, scale_m)


def feed_part(rows, up_ref, down_ref):
    hidden = jax.nn.gelu(dot(rows, up_ref[...]), approximate=True).astype(BF16)
    return dot_t(down_ref[...], hidden)


def feed_first_body(rows_ref, up_ref, down_ref, sum_ref):
    @pl.when(pl.program_id(0) == 0)
    def _():
        sum_ref[...] = jnp.zeros(sum_ref.shape, F32)

    sum_ref[...] += feed_part(rows_ref[...], up_ref, down_ref)


def feed_second_body(own_ref, pair_ref, up_ref, down_ref, before_ref, pair_before_ref,
                     keep_ref, send_ref, rows_ref, sum_ref):
    count = own_ref.shape[0]

    @pl.when(pl.program_id(0) == 0)
    def _():
        rows_ref[:count] = own_ref[...]
        rows_ref[count:] = pair_ref[...]
        sum_ref[:, :count] = before_ref[...]
        sum_ref[:, count:] = pair_before_ref[...]

    sum_ref[...] += feed_part(rows_ref[...], up_ref, down_ref)

    @pl.when(pl.program_id(0) == pl.num_programs(0) - 1)
    def _():
        total = sum_ref[...].T
        keep_ref[...] = total[:count]
        send_ref[...] = total[count:].astype(BF16)


def feed_first(rows, weights):
    count, width = rows.shape
    steps = 3
    up = pl.BlockSpec((width, width // steps), lambda i: (0, steps + i))
    down = pl.BlockSpec((width, width // steps), lambda i: (0, i))
    return pl.pallas_call(
        feed_first_body,
        grid=(steps,),
        in_specs=[whole(rows.shape), up, down],
        out_specs=whole((width, count)),
        out_shape=jax.ShapeDtypeStruct((width, count), F32),
        name="feed_first",
        compiler_params=pltpu.CompilerParams(vmem_limit_bytes=20 << 20),
    )(rows, weights, weights)


def feed_second(own, pair, weights, before, pair_before):
    count, width = own.shape
    steps = 3
    up = pl.BlockSpec((width, width // steps), lambda i: (0, steps + i))
    down = pl.BlockSpec((width, width // steps), lambda i: (0, i))
    return pl.pallas_call(
        feed_second_body,
        grid=(steps,),
        in_specs=[
            whole(own.shape),
            whole(own.shape),
            up,
            down,
            whole(before.shape),
            whole(before.shape),
        ],
        out_specs=[whole(own.shape), whole(own.shape)],
        out_shape=[
            jax.ShapeDtypeStruct(own.shape, F32),
            jax.ShapeDtypeStruct(own.shape, BF16),
        ],
        scratch_shapes=[pltpu.VMEM((2 * count, width), BF16), pltpu.VMEM((width, 2 * count), F32)],
        name="feed_second",
        compiler_params=pltpu.CompilerParams(vmem_limit_bytes=20 << 20),
    )(own, pair, weights, weights, before, pair_before)


def finish_body(scale_by_ref, keep_ref, recv_ref, first_ref, gate_ref, shift_ref, scale_ref, out_w_ref, out_ref):
    share = first_ref.shape[1]
    noise = []
    for i in range(2):
        part = slice(i * share, (i + 1) * share)
        mlp = keep_ref[part] + recv_ref[part].astype(F32)
        total = first_ref[i] + gate_ref[i] * mlp
        fin = (layer_norm(total) * (1.0 + scale_ref[i]) + shift_ref[i]).astype(BF16)
        noise.append(dot(fin, out_w_ref[...]))
    guided = noise[1] + scale_by_ref[0] * (noise[0] - noise[1])
    outs = guided.shape[1]
    wide = jnp.concatenate([guided] * (128 // outs), axis=1)
    wide = jnp.concatenate([wide] * (share * outs // 128), axis=1)
    token = lax.broadcasted_iota(jnp.int32, wide.shape, 0)
    mine = lax.broadcasted_iota(jnp.int32, wide.shape, 1) // outs == token
    out_ref[...] = jnp.sum(jnp.where(mine, wide, 0.0), axis=0, keepdims=True)


def finish(guidance, keep, recv, first_sum, gate_m, shift_f, scale_f, out_local):
    _, share, width = first_sum.shape
    vector = whole((2, 1, width))
    return pl.pallas_call(
        finish_body,
        grid_spec=pltpu.PrefetchScalarGridSpec(
            num_scalar_prefetch=1,
            grid=(1,),
            in_specs=[
                whole(keep.shape),
                whole(recv.shape),
                whole(first_sum.shape),
                vector,
                vector,
                vector,
                whole(out_local.shape),
            ],
            out_specs=whole((1, share * out_local.shape[1])),
        ),
        out_shape=jax.ShapeDtypeStruct((1, share * out_local.shape[1]), F32),
        name="finish",
        compiler_params=pltpu.CompilerParams(vmem_limit_bytes=20 << 20),
    )(guidance, keep, recv, first_sum, gate_m, shift_f, scale_f, out_local)


def on_device(
    x_arrive,
    cond_first,
    labels,
    step_ids,
    guidance,
    time_table,
    class_table,
    ada_weight,
    final_ada,
    qkv_weight,
    proj_weight,
    fc1_weight,
    fc2_weight,
    out_weight,
):
    tokens = x_arrive.shape[1]
    width = x_arrive.shape[2]
    rows = qkv_weight.shape[1]
    quarter = qkv_weight.shape[2]
    core = lax.axis_index("group")
    column = lax.axis_index("dp_1")
    high = lax.axis_index("dp_2")
    place = lax.axis_index("mp")
    n_y, n_x, n_z = (lax.axis_size(axis) for axis in DP)
    n_mp = lax.axis_size("mp")
    half = quarter // 2

    time_part = jnp.take(time_table, step_ids, axis=0).astype(F32)
    class_part = jnp.take(class_table, labels, axis=0).astype(F32)
    null_part = class_table[CLASSES].astype(F32)[None, :]
    acts = jax.nn.silu(jnp.concatenate([time_part + class_part, time_part + null_part])).astype(BF16)
    every_act = to_everyone(acts, DP).reshape(-1, acts.shape[1])

    qkv_own = jnp.where(core == 0, qkv_weight[:, :, :half], qkv_weight[:, :, half:])
    qkv_own = qkv_own.transpose(1, 0, 2).reshape(rows, 3 * half)

    shards = jnp.concatenate([fc2_weight.T, fc1_weight, proj_weight.T, qkv_own], axis=1)
    shards = by_height(shards, swap(shards, "dp_2", 1), high)
    qkv_block = shards[:, 2 * width + quarter :]

    def fetch(x, along):
        pairs = [(c * n_mp + m, c * n_mp + (m ^ (2 * c) ^ along)) for c in range(2) for m in range(n_mp)]
        return lax.ppermute(x, ("group", "mp"), pairs)

    feed = fetch(shards[:, : 2 * width + quarter], 0)
    proj_beside = fetch(shards[:, 2 * width : 2 * width + quarter], 1)
    part_a = lanes_full(jnp.concatenate([qkv_block, feed[:, 2 * width :], proj_beside], axis=1))
    part_a, every_act = lax.optimization_barrier((part_a, every_act))
    part_a = gather_y(part_a)
    part_a, every_act = lax.optimization_barrier((part_a, every_act))
    part_a = gather_x(part_a)
    other_a = swap(part_a, "group", 1)

    wide = max(2 * width, -(-GATHER_FLOOR // (2 * n_x * feed.shape[0] * 128)) * 128)
    feed = jnp.pad(feed[:, : 2 * width], ((0, 0), (0, wide - 2 * width)))
    feed = lax.all_gather(feed, "dp_1", axis=0)
    feed = feed[:, :, : 2 * width].reshape(-1, 2 * width)
    feed = lax.all_gather(feed, "dp_0", axis=0, tiled=True)
    other_feed = swap(feed, "group", 1)

    mod_part = dot(every_act, ada_weight).astype(BF16)
    mod_part = lax.all_to_all(mod_part, DP, split_axis=0, concat_axis=1, tiled=True)
    final_part = dot(acts, final_ada).astype(BF16)
    mod_parts = to_everyone(jnp.concatenate([mod_part, final_part], axis=1), "mp")

    spot = lax.broadcasted_iota(jnp.int32, (1, width), 1)
    per_x = n_y * n_z * rows
    per_y = n_z * rows
    block = spot // per_x
    inside = spot % per_x
    offset = jnp.where(block == 1, n_x - 1, jnp.where(block == 2, 1, jnp.where(block == 3, 2, 0)))

    from_x = (column + offset) % n_x
    final = (inside // per_y * n_x + from_x) * per_y + inside % per_y
    near_order = (lax.broadcasted_iota(jnp.int32, (width, width), 0) == final).astype(BF16)
    change = (final.reshape(width, 1) == spot).astype(BF16)

    first = cond_first[0] == 1
    cond_rows = jnp.where(first, x_arrive[0], x_arrive[1])
    uncond_rows = jnp.where(first, x_arrive[1], x_arrive[0])
    arrived = jnp.stack([cond_rows, uncond_rows])
    share = tokens // n_mp
    own = lax.dynamic_slice_in_dim(arrived, place * share, share, 1)
    images = dot(arrived.reshape(-1, width), near_order).astype(BF16)
    images = images.reshape(2, tokens, width)
    mod_parts = mod_parts.reshape(n_mp * 2, -1, width)

    turned = dot(mod_parts[:, :2].reshape(-1, width), near_order).reshape(n_mp, 2, 2, 1, width)
    turned = jnp.sum(turned, axis=0)
    shift_a, scale_a = turned[:, 0], turned[:, 1]
    mods = mod_parts[:, 2:].astype(F32).reshape(n_mp, 2, -1, 1, width)
    mods = jnp.sum(mods, axis=0)
    gate_a, shift_m, scale_m, gate_m, shift_f, scale_f = (mods[:, i] for i in range(6))

    cores = core.reshape(1).astype(jnp.int32)
    mixed = attention(cores, images, shift_a, scale_a, part_a, other_a, n_mp, quarter)
    mixed = lax.all_to_all(mixed, "mp", 0, 0, tiled=True)
    base = (place ^ (2 * core)).reshape(1).astype(jnp.int32)
    first_sum, hidden_two = project(base, mixed, part_a, other_a, change, own, gate_a, shift_m, scale_m)
    hidden_two = hidden_two.reshape(2 * share, width)
    pair = swap(hidden_two, "mp", 1)
    before = feed_first(hidden_two, feed)
    pair_before = feed_first(pair, feed)
    keep, send = feed_second(hidden_two, pair, other_feed, before, pair_before)
    recv = swap(send, "mp", 1)
    return finish(guidance, keep, recv, first_sum, gate_m, shift_f, scale_f, out_weight)


def solution(mesh):
    torus = Mesh(
        mesh.devices.reshape(mesh.shape["group"], 8, 4, 2, mesh.shape["mp"]),
        ("group", "dp_0", "dp_1", "dp_2", "mp"),
    )
    placed = (
        P(GROUP_DP, None, None),
        P(GROUP_DP),
        P(GROUP_DP),
        P(GROUP_DP),
        P(),
        P(None, "mp"),
        P(None, "mp"),
        P("mp", DP),
        P("mp", None),
        P(None, DP, "mp"),
        P("mp", DP),
        P(DP, "mp"),
        P("mp", DP),
        P(),
    )
    return jax.shard_map(
        on_device, mesh=torus, in_specs=placed, out_specs=P(GROUP_DP, "mp"), check_vma=False
    )
```

```python
import jax
import jax.numpy as jnp
from jax import lax
from jax.experimental import pallas as pl
from jax.experimental.pallas import tpu as pltpu
from jax.sharding import Mesh
from jax.sharding import PartitionSpec as P

CLASSES = 1000
GATHER_FLOOR = 1 << 20
DP = ("dp_0", "dp_1", "dp_2")
GROUP_DP = ("group", "dp_0", "dp_1", "dp_2")
BF16 = jnp.bfloat16
F32 = jnp.float32


def to_everyone(x, axis):
    size = lax.axis_size(axis)
    return lax.all_to_all(jnp.broadcast_to(x[None], (size, *x.shape)), axis, 0, 0, tiled=True)


def shift(x, axis, step):
    size = lax.axis_size(axis)
    return lax.ppermute(x, axis, [(i, (i + step) % size) for i in range(size)])


def swap(x, axis, bit):
    size = lax.axis_size(axis)
    return lax.ppermute(x, axis, [(i, i ^ bit) for i in range(size)])


def gather_y(block):
    pieces = to_everyone(block, "dp_0")
    return pieces.reshape(pieces.shape[0] * pieces.shape[1], pieces.shape[2])


def gather_x(block):
    half = block.shape[0] // 2
    left = shift(block, "dp_1", 1)
    right = shift(block, "dp_1", -1)
    top, bottom = left[:half], right[half:]
    left, right, top, bottom = lax.optimization_barrier((left, right, top, bottom))
    far_top = shift(top, "dp_1", 1)
    far_bottom = shift(bottom, "dp_1", -1)
    return jnp.concatenate([block, left, right, far_top, far_bottom], axis=0)


def by_height(own, other, high):
    own_low = high == 0
    return jnp.concatenate([jnp.where(own_low, own, other), jnp.where(own_low, other, own)])


def lanes_full(x):
    return jnp.pad(x, ((0, 0), (0, -x.shape[1] % 128)))


def layer_norm(values):
    mean = jnp.mean(values, axis=-1, keepdims=True)
    centred = values - mean
    spread = jnp.mean(centred * centred, axis=-1, keepdims=True)
    return centred * lax.rsqrt(spread + 1e-06)


def dot(a, b):
    return jnp.dot(a, b, preferred_element_type=F32)


def dot_t(a, b):
    return lax.dot_general(a, b, (((1,), (1,)), ((), ())), preferred_element_type=F32)


def whole(shape):
    return pl.BlockSpec(shape, lambda *_: (0,) * len(shape))


def attention_body(core_ref, x_ref, shift_ref, scale_ref, mine_ref, other_ref, out_ref):
    images, tokens, _ = x_ref.shape
    pieces, quarter, _ = out_ref.shape
    head_dim = quarter // 4
    share = tokens // pieces
    scale = head_dim ** (-0.5)
    low = core_ref[0] == 0
    for image in range(images):
        x = x_ref[image].astype(F32)
        hidden = (layer_norm(x) * (1.0 + scale_ref[image]) + shift_ref[image]).astype(BF16)
        sides = []
        for ref in (mine_ref, other_ref):
            qkv = dot(hidden, ref[:, : 6 * head_dim]).astype(BF16)
            heads = []
            for head in range(2):
                at = head * head_dim
                query = qkv[:, at : at + head_dim]
                keys = qkv[:, 2 * head_dim + at : 3 * head_dim + at]
                values = qkv[:, 4 * head_dim + at : 5 * head_dim + at]
                scores = dot_t(query, keys) * scale
                top = jnp.max(scores, axis=-1, keepdims=True)
                weights = jnp.exp(scores - top)
                total = jnp.sum(weights, axis=-1, keepdims=True)
                probs = (weights * (1.0 / total)).astype(BF16)
                mixed = lax.dot_general(
                    values, probs, (((0,), (1,)), ((), ())), preferred_element_type=F32
                )
                heads.append(mixed.astype(BF16))
            sides.append(jnp.concatenate(heads, axis=0))
        first = jnp.where(low, sides[0], sides[1])
        second = jnp.where(low, sides[1], sides[0])
        mixed = jnp.concatenate([first, second], axis=0)
        for piece in range(pieces):
            part = mixed[:, piece * share : (piece + 1) * share]
            out_ref[piece, :, image * share : (image + 1) * share] = part


def attention(core, x, shift_a, scale_a, mine, other, n_mp, quarter):
    images, tokens, width = x.shape
    vector = whole((images, 1, width))
    out_shape = (n_mp, quarter, images * tokens // n_mp)
    lanes = whole((width, -(-3 * quarter // 2 // 128) * 128))
    return pl.pallas_call(
        attention_body,
        grid_spec=pltpu.PrefetchScalarGridSpec(
            num_scalar_prefetch=1,
            grid=(1,),
            in_specs=[whole(x.shape), vector, vector, lanes, lanes],
            out_specs=whole(out_shape),
        ),
        out_shape=jax.ShapeDtypeStruct(out_shape, BF16),
        name="attention",
        compiler_params=pltpu.CompilerParams(vmem_limit_bytes=20 << 20),
    )(core, x, shift_a, scale_a, mine, other)


def project_body(base_ref, mixed_ref, mine_ref, other_ref, change_ref, own_ref, gate_ref, shift_ref, scale_ref,
                 sum_ref, hidden_ref, rows_ref):
    quarter = mixed_ref.shape[1]
    start = 3 * quarter // 2
    lead = start % 128
    base = base_ref[0]
    rows_ref[...] = jnp.zeros(rows_ref.shape, BF16)
    for i in range(4):
        at = lead + i % 2 * quarter
        rows_ref[i // 2, at : at + quarter] = mixed_ref[base ^ i]
    attn = dot(mine_ref[...], rows_ref[0])
    attn = (attn + dot(other_ref[...], rows_ref[1])).astype(BF16)
    attn = lax.dot_general(
        attn, change_ref[...], (((0,), (0,)), ((), ())), preferred_element_type=F32
    )
    share = own_ref.shape[1]
    for i in range(2):
        total = own_ref[i].astype(F32) + gate_ref[i] * attn[i * share : (i + 1) * share]
        sum_ref[i] = total
        hidden_ref[i] = (layer_norm(total) * (1.0 + scale_ref[i]) + shift_ref[i]).astype(BF16)


def project(base, mixed, mine, other, change, own, gate_a, shift_m, scale_m):
    _, share, width = own.shape
    vector = whole((2, 1, width))
    start = 3 * mixed.shape[1] // 2
    depth = mine.shape[1] - start // 128 * 128
    lanes = pl.BlockSpec(
        (pl.Element(width), pl.Element(depth)), lambda *_: (0, start // 128 * 128)
    )
    return pl.pallas_call(
        project_body,
        grid_spec=pltpu.PrefetchScalarGridSpec(
            num_scalar_prefetch=1,
            grid=(1,),
            in_specs=[
                whole(mixed.shape),
                lanes,
                lanes,
                whole(change.shape),
                whole(own.shape),
                vector,
                vector,
                vector,
            ],
            out_specs=[whole(own.shape), whole(own.shape)],
            scratch_shapes=[pltpu.VMEM((2, depth, 2 * share), BF16)],
        ),
        out_shape=[
            jax.ShapeDtypeStruct(own.shape, F32),
            jax.ShapeDtypeStruct(own.shape, BF16),
        ],
        name="project",
        compiler_params=pltpu.CompilerParams(vmem_limit_bytes=20 << 20),
    )(base, mixed, mine, other, change, own, gate_a, shift_m, scale_m)


def feed_part(rows, up_ref, down_ref):
    hidden = jax.nn.gelu(dot(rows, up_ref[...]), approximate=True).astype(BF16)
    return dot_t(down_ref[...], hidden)


def feed_first_body(rows_ref, up_ref, down_ref, sum_ref):
    @pl.when(pl.program_id(0) == 0)
    def _():
        sum_ref[...] = jnp.zeros(sum_ref.shape, F32)

    sum_ref[...] += feed_part(rows_ref[...], up_ref, down_ref)


def feed_second_body(own_ref, pair_ref, up_ref, down_ref, before_ref, pair_before_ref,
                     keep_ref, send_ref, rows_ref, sum_ref):
    count = own_ref.shape[0]

    @pl.when(pl.program_id(0) == 0)
    def _():
        rows_ref[:count] = own_ref[...]
        rows_ref[count:] = pair_ref[...]
        sum_ref[:, :count] = before_ref[...]
        sum_ref[:, count:] = pair_before_ref[...]

    sum_ref[...] += feed_part(rows_ref[...], up_ref, down_ref)

    @pl.when(pl.program_id(0) == pl.num_programs(0) - 1)
    def _():
        total = sum_ref[...].T
        keep_ref[...] = total[:count]
        send_ref[...] = total[count:].astype(BF16)


def feed_first(rows, weights):
    count, width = rows.shape
    steps = 3
    up = pl.BlockSpec((width, width // steps), lambda i: (0, steps + i))
    down = pl.BlockSpec((width, width // steps), lambda i: (0, i))
    return pl.pallas_call(
        feed_first_body,
        grid=(steps,),
        in_specs=[whole(rows.shape), up, down],
        out_specs=whole((width, count)),
        out_shape=jax.ShapeDtypeStruct((width, count), F32),
        name="feed_first",
        compiler_params=pltpu.CompilerParams(vmem_limit_bytes=20 << 20),
    )(rows, weights, weights)


def feed_second(own, pair, weights, before, pair_before):
    count, width = own.shape
    steps = 3
    up = pl.BlockSpec((width, width // steps), lambda i: (0, steps + i))
    down = pl.BlockSpec((width, width // steps), lambda i: (0, i))
    return pl.pallas_call(
        feed_second_body,
        grid=(steps,),
        in_specs=[
            whole(own.shape),
            whole(own.shape),
            up,
            down,
            whole(before.shape),
            whole(before.shape),
        ],
        out_specs=[whole(own.shape), whole(own.shape)],
        out_shape=[
            jax.ShapeDtypeStruct(own.shape, F32),
            jax.ShapeDtypeStruct(own.shape, BF16),
        ],
        scratch_shapes=[pltpu.VMEM((2 * count, width), BF16), pltpu.VMEM((width, 2 * count), F32)],
        name="feed_second",
        compiler_params=pltpu.CompilerParams(vmem_limit_bytes=20 << 20),
    )(own, pair, weights, weights, before, pair_before)


def finish_body(scale_by_ref, keep_ref, recv_ref, first_ref, gate_ref, shift_ref, scale_ref, out_w_ref, out_ref):
    share = first_ref.shape[1]
    noise = []
    for i in range(2):
        part = slice(i * share, (i + 1) * share)
        mlp = keep_ref[part] + recv_ref[part].astype(F32)
        total = first_ref[i] + gate_ref[i] * mlp
        fin = (layer_norm(total) * (1.0 + scale_ref[i]) + shift_ref[i]).astype(BF16)
        noise.append(dot(fin, out_w_ref[...]))
    guided = noise[1] + scale_by_ref[0] * (noise[0] - noise[1])
    outs = guided.shape[1]
    wide = jnp.concatenate([guided] * (128 // outs), axis=1)
    wide = jnp.concatenate([wide] * (share * outs // 128), axis=1)
    token = lax.broadcasted_iota(jnp.int32, wide.shape, 0)
    mine = lax.broadcasted_iota(jnp.int32, wide.shape, 1) // outs == token
    out_ref[...] = jnp.sum(jnp.where(mine, wide, 0.0), axis=0, keepdims=True)


def finish(guidance, keep, recv, first_sum, gate_m, shift_f, scale_f, out_local):
    _, share, width = first_sum.shape
    vector = whole((2, 1, width))
    return pl.pallas_call(
        finish_body,
        grid_spec=pltpu.PrefetchScalarGridSpec(
            num_scalar_prefetch=1,
            grid=(1,),
            in_specs=[
                whole(keep.shape),
                whole(recv.shape),
                whole(first_sum.shape),
                vector,
                vector,
                vector,
                whole(out_local.shape),
            ],
            out_specs=whole((1, share * out_local.shape[1])),
        ),
        out_shape=jax.ShapeDtypeStruct((1, share * out_local.shape[1]), F32),
        name="finish",
        compiler_params=pltpu.CompilerParams(vmem_limit_bytes=20 << 20),
    )(guidance, keep, recv, first_sum, gate_m, shift_f, scale_f, out_local)


def on_device(
    x_arrive,
    cond_first,
    labels,
    step_ids,
    guidance,
    time_table,
    class_table,
    ada_weight,
    final_ada,
    qkv_weight,
    proj_weight,
    fc1_weight,
    fc2_weight,
    out_weight,
):
    tokens = x_arrive.shape[1]
    width = x_arrive.shape[2]
    rows = qkv_weight.shape[1]
    quarter = qkv_weight.shape[2]
    core = lax.axis_index("group")
    column = lax.axis_index("dp_1")
    high = lax.axis_index("dp_2")
    place = lax.axis_index("mp")
    n_y, n_x, n_z = (lax.axis_size(axis) for axis in DP)
    n_mp = lax.axis_size("mp")
    half = quarter // 2

    time_part = jnp.take(time_table, step_ids, axis=0).astype(F32)
    class_part = jnp.take(class_table, labels, axis=0).astype(F32)
    null_part = class_table[CLASSES].astype(F32)[None, :]
    acts = jax.nn.silu(jnp.concatenate([time_part + class_part, time_part + null_part])).astype(BF16)
    every_act = to_everyone(acts, DP).reshape(-1, acts.shape[1])

    qkv_own = jnp.where(core == 0, qkv_weight[:, :, :half], qkv_weight[:, :, half:])
    qkv_own = qkv_own.transpose(1, 0, 2).reshape(rows, 3 * half)

    shards = jnp.concatenate([fc2_weight.T, fc1_weight, proj_weight.T, qkv_own], axis=1)
    shards = by_height(shards, swap(shards, "dp_2", 1), high)
    qkv_block = shards[:, 2 * width + quarter :]

    def fetch(x, along):
        pairs = [(c * n_mp + m, c * n_mp + (m ^ (2 * c) ^ along)) for c in range(2) for m in range(n_mp)]
        return lax.ppermute(x, ("group", "mp"), pairs)

    feed = fetch(shards[:, : 2 * width + quarter], 0)
    proj_beside = fetch(shards[:, 2 * width : 2 * width + quarter], 1)
    part_a = lanes_full(jnp.concatenate([qkv_block, feed[:, 2 * width :], proj_beside], axis=1))
    part_a, every_act = lax.optimization_barrier((part_a, every_act))
    part_a = gather_y(part_a)
    part_a, every_act = lax.optimization_barrier((part_a, every_act))
    part_a = gather_x(part_a)
    other_a = swap(part_a, "group", 1)

    wide = max(2 * width, -(-GATHER_FLOOR // (2 * n_x * feed.shape[0] * 128)) * 128)
    feed = jnp.pad(feed[:, : 2 * width], ((0, 0), (0, wide - 2 * width)))
    feed = lax.all_gather(feed, "dp_1", axis=0)
    feed = feed[:, :, : 2 * width].reshape(-1, 2 * width)
    feed = lax.all_gather(feed, "dp_0", axis=0, tiled=True)
    other_feed = swap(feed, "group", 1)

    mod_part = dot(every_act, ada_weight).astype(BF16)
    mod_part = lax.all_to_all(mod_part, DP, split_axis=0, concat_axis=1, tiled=True)
    final_part = dot(acts, final_ada).astype(BF16)
    mod_parts = to_everyone(jnp.concatenate([mod_part, final_part], axis=1), "mp")

    spot = lax.broadcasted_iota(jnp.int32, (1, width), 1)
    per_x = n_y * n_z * rows
    per_y = n_z * rows
    block = spot // per_x
    inside = spot % per_x
    offset = jnp.where(block == 1, n_x - 1, jnp.where(block == 2, 1, jnp.where(block == 3, 2, 0)))

    from_x = (column + offset) % n_x
    final = (inside // per_y * n_x + from_x) * per_y + inside % per_y
    near_order = (lax.broadcasted_iota(jnp.int32, (width, width), 0) == final).astype(BF16)
    change = (final.reshape(width, 1) == spot).astype(BF16)

    first = cond_first[0] == 1
    cond_rows = jnp.where(first, x_arrive[0], x_arrive[1])
    uncond_rows = jnp.where(first, x_arrive[1], x_arrive[0])
    arrived = jnp.stack([cond_rows, uncond_rows])
    share = tokens // n_mp
    own = lax.dynamic_slice_in_dim(arrived, place * share, share, 1)
    images = dot(arrived.reshape(-1, width), near_order).astype(BF16)
    images = images.reshape(2, tokens, width)
    mod_parts = mod_parts.reshape(n_mp * 2, -1, width)

    turned = dot(mod_parts[:, :2].reshape(-1, width), near_order).reshape(n_mp, 2, 2, 1, width)
    turned = jnp.sum(turned, axis=0)
    shift_a, scale_a = turned[:, 0], turned[:, 1]
    mods = mod_parts[:, 2:].astype(F32).reshape(n_mp, 2, -1, 1, width)
    mods = jnp.sum(mods, axis=0)
    gate_a, shift_m, scale_m, gate_m, shift_f, scale_f = (mods[:, i] for i in range(6))

    cores = core.reshape(1).astype(jnp.int32)
    mixed = attention(cores, images, shift_a, scale_a, part_a, other_a, n_mp, quarter)
    mixed = lax.all_to_all(mixed, "mp", 0, 0, tiled=True)
    base = (place ^ (2 * core)).reshape(1).astype(jnp.int32)
    first_sum, hidden_two = project(base, mixed, part_a, other_a, change, own, gate_a, shift_m, scale_m)
    hidden_two = hidden_two.reshape(2 * share, width)
    pair = swap(hidden_two, "mp", 1)
    before = feed_first(hidden_two, feed)
    pair_before = feed_first(pair, feed)
    keep, send = feed_second(hidden_two, pair, other_feed, before, pair_before)
    recv = swap(send, "mp", 1)
    return finish(guidance, keep, recv, first_sum, gate_m, shift_f, scale_f, out_weight)


def solution(mesh):
    torus = Mesh(
        mesh.devices.reshape(mesh.shape["group"], 8, 4, 2, mesh.shape["mp"]),
        ("group", "dp_0", "dp_1", "dp_2", "mp"),
    )
    placed = (
        P(GROUP_DP, None, None),
        P(GROUP_DP),
        P(GROUP_DP),
        P(GROUP_DP),
        P(),
        P(None, "mp"),
        P(None, "mp"),
        P("mp", DP),
        P("mp", None),
        P(None, DP, "mp"),
        P("mp", DP),
        P(DP, "mp"),
        P("mp", DP),
        P(),
    )
    return jax.shard_map(
        on_device, mesh=torus, in_specs=placed, out_specs=P(GROUP_DP, "mp"), check_vma=False
    )
```
